128 devices in a mesh: rep: 16 (over y_hi, z, core), tp: 8 (over y_lo, x).
Axes of the slice: x: 4, y: 4 (y_hi: 2, y_lo: 2; y = y_hi * 2 + y_lo), z: 4, core: 2. Of those that a mesh axis runs over, the one named last changes fastest.
Arguments:
- delta_query: bfloat16 [16, 2, 2048, 3072], P('rep', None, None, 'tp'), may hold values from -6 to 6
- master_query: float32 [2, 2048, 3072], P(None, 'rep', 'tp'), may hold values from -3 to 3
- moment_query: float32 [2, 2048, 3072], P(None, 'rep', 'tp'), may hold values from -3 to 3
- delta_latent: bfloat16 [16, 2, 512, 4096], P('rep', None, None, 'tp'), may hold values from -6 to 6
- master_latent: float32 [2, 512, 4096], P(None, 'rep', 'tp'), may hold values from -3 to 3
- moment_latent: float32 [2, 512, 4096], P(None, 'rep', 'tp'), may hold values from -3 to 3
- delta_output: bfloat16 [16, 2, 2048, 2048], P('rep', None, 'tp'), may hold values from -6 to 6
- master_output: float32 [2, 2048, 2048], P(None, 'tp', 'rep'), may hold values from -3 to 3
- moment_output: float32 [2, 2048, 2048], P(None, 'tp', 'rep'), may hold values from -3 to 3
Outputs:
- params_query: bfloat16 [2, 2048, 3072], P(None, None, 'tp')
- new_master_query: float32 [2, 2048, 3072], P(None, 'rep', 'tp')
- new_moment_query: float32 [2, 2048, 3072], P(None, 'rep', 'tp')
- params_latent: bfloat16 [2, 512, 4096], P(None, None, 'tp')
- new_master_latent: float32 [2, 512, 4096], P(None, 'rep', 'tp')
- new_moment_latent: float32 [2, 512, 4096], P(None, 'rep', 'tp')
- params_output: bfloat16 [2, 2048, 2048], P(None, 'tp')
- new_master_output: float32 [2, 2048, 2048], P(None, 'tp', 'rep')
- new_moment_output: float32 [2, 2048, 2048], P(None, 'tp', 'rep')
The draws below stay inside these ranges and needn't reach their ends.
All inputs are finite; a program needn't handle non-finite values.
Results may differ from the reference program's by a relative error of at most 0.012.
Values may be sent and summed in bfloat16 or wider, within the bound.
A program may use at most 64 MiB of HBM per device.

```python
import jax
import jax.numpy as jnp
from jax import lax

D = 2048
KV_RANK = 512
LAYERS = 2
REPLICAS = 16
QCOLS = 3072
KVCOLS = 4096
OROWS = 2048


def spiked(drawn, rng, source, target, blocks, factor):
    owner, partner = [(jnp.arange(drawn.shape[dim]) // (drawn.shape[dim] // blocks)).reshape([-1 if axis == dim else 1 for axis in range(drawn.ndim)]) for dim in (source, target)]
    chosen = jax.random.permutation(rng, blocks)[partner]
    strong = (owner == chosen) | (owner == (partner + blocks // 2) % blocks)
    return jnp.where(strong, factor * drawn, drawn)


def level_of(own_key, dims, pieces, smallest, top_value):
    loudness = 1.0
    for dim, parts in pieces:
        steps = jax.random.uniform(jax.random.fold_in(jax.random.fold_in(own_key, 6), dim), (parts,), jnp.float32, smallest / len(pieces), top_value / len(pieces))
        loudness = loudness * jnp.repeat(jnp.exp(steps), dims[dim] // parts).reshape((-1,) + (1,) * (len(dims) - 1 - dim))
    return loudness


def gaussian(own_key, extent, scale, bound, shards=(), kind=jnp.bfloat16):
    drawn = jax.random.normal(own_key, extent, jnp.float32) * scale
    if len(shards) > 0:
        drawn = level_of(own_key, extent, shards, -0.22, 0.18) * drawn
    return jnp.clip(drawn, min=-bound, max=bound).astype(kind)


def noise_with(rng, dims, deviation, limit, shards, heavy, held_as=jnp.bfloat16):
    entries = deviation * jax.random.normal(rng, dims, jnp.float32)
    if shards:
        entries = entries * level_of(rng, dims, shards, -0.22, 0.18)
    return jnp.clip(spiked(entries, jax.random.fold_in(rng, 3), *heavy), -limit, limit).astype(held_as)


def setup_inputs(seed: int = 0) -> dict:
    streams_of = jax.random.split(jax.random.key(seed), 10)
    delta_query = noise_with(streams_of[0], (REPLICAS, LAYERS, D, QCOLS), 1.0, 6.0, ((0, 16), (3, 8)), (0, 2, 16, 2.0))
    master_query = gaussian(streams_of[1], (LAYERS, D, QCOLS), 0.5, 3.0, ((1, 16), (2, 8)), jnp.float32)
    moment_query = gaussian(streams_of[2], (LAYERS, D, QCOLS), 0.3, 3.0, ((1, 16), (2, 8)), jnp.float32)
    delta_latent = noise_with(streams_of[3], (REPLICAS, LAYERS, KV_RANK, KVCOLS), 1.0, 6.0, ((0, 16), (3, 8)), (0, 2, 16, 2.0))
    master_latent = gaussian(streams_of[4], (LAYERS, KV_RANK, KVCOLS), 0.5, 3.0, ((1, 16), (2, 8)), jnp.float32)
    moment_latent = gaussian(streams_of[5], (LAYERS, KV_RANK, KVCOLS), 0.3, 3.0, ((1, 16), (2, 8)), jnp.float32)
    delta_output = noise_with(streams_of[6], (REPLICAS, LAYERS, OROWS, D), 1.0, 6.0, ((0, 16), (2, 8)), (0, 3, 16, 2.0))
    master_output = gaussian(streams_of[7], (LAYERS, OROWS, D), 0.5, 3.0, ((1, 8), (2, 16)), jnp.float32)
    moment_output = gaussian(streams_of[8], (LAYERS, OROWS, D), 0.3, 3.0, ((1, 8), (2, 16)), jnp.float32)
    return dict(delta_query=delta_query, master_query=master_query, moment_query=moment_query, delta_latent=delta_latent, master_latent=master_latent, moment_latent=moment_latent, delta_output=delta_output, master_output=master_output, moment_output=moment_output)


OUTER_RATE = 0.7
OUTER_MOMENTUM = 0.9


def accumulate(delta):
    def add_replica(replica, running):
        return running + delta[replica].astype(jnp.float32)

    return lax.fori_loop(0, REPLICAS, add_replica, jnp.zeros(delta.shape[1:], jnp.float32))


def update(delta, master, moment):
    average = accumulate(delta) / REPLICAS
    momentum = OUTER_MOMENTUM * moment + average
    updated = master - OUTER_RATE * (average + OUTER_MOMENTUM * momentum)
    return updated.astype(jnp.bfloat16), updated, momentum


def reference(delta_query, master_query, moment_query, delta_latent, master_latent, moment_latent, delta_output, master_output, moment_output):
    query_params, query_master, query_moment = update(delta_query, master_query, moment_query)
    latent_params, latent_master, latent_moment = update(delta_latent, master_latent, moment_latent)
    output_params, output_master, output_moment = update(delta_output, master_output, moment_output)
    return (query_params, query_master, query_moment, latent_params, latent_master, latent_moment, output_params, output_master, output_moment)
```

```python
import jax
import jax.numpy as jnp
from jax import lax
from jax.experimental import pallas as pl
from jax.experimental.pallas import tpu as pltpu
from jax.sharding import Mesh
from jax.sharding import PartitionSpec as P

REP = ("yh", "z", "c")
TP = ("yl", "x")
MESH = pl.DeviceIdType.MESH

OUTER_RATE = 0.7
OUTER_MOMENTUM = 0.9
REPLICAS = 16

BLOCKS = ((128, 384), (32, 512), (256, 128))
LAYERS = 2
Z_FIRST = ((0, 0), (0, 1))
Y_FIRST = ((1, 0), (1, 1), (2, 0), (2, 1))
COPIES = 256
LOADS = 64


def outer_kernel(*refs):
    f32, bf16 = jnp.float32, jnp.bfloat16
    delta, master, moment = refs[0:9:3], refs[1:9:3], refs[2:9:3]
    params, new_master, new_moment = refs[9:18:3], refs[10:18:3], refs[11:18:3]
    own, peer, far, direct, summed, across, held_master, held_moment = (
        refs[18 + 3 * i : 21 + 3 * i] for i in range(8)
    )
    load_sem, send_sem, recv_sem = refs[42:]

    yh, z, c = (lax.axis_index(a) for a in REP)
    zs = [lax.rem(z + k, 4) for k in range(4)]
    ys = [yh, 1 - yh]
    core_to, y_to = {"c": 1 - c}, {"yh": 1 - yh}

    def up(layer):
        return 1 if layer == 0 else 3

    def down(layer):
        return 3 if layer == 0 else 1

    started, loads = [], []

    def send(src, dst, to):
        i = len(started)
        copy = pltpu.make_async_remote_copy(
            src_ref=src,
            dst_ref=dst,
            send_sem=send_sem.at[i],
            recv_sem=recv_sem.at[i],
            device_id=to,
            device_id_type=MESH,
        )
        copy.start()
        started.append(copy)
        return copy

    def load(src, dst):
        copy = pltpu.make_async_copy(src, dst, load_sem.at[len(loads)])
        copy.start()
        loads.append(copy)
        return copy

    def block(ref, a, layer, y, zz, core):
        if a < 2:
            return ref[a].at[layer, y, zz, core]
        column = pl.multiple_of(((y * 4 + zz) * 2 + core) * 128, 128)
        return ref[2].at[layer, :, pl.ds(column, 128)]

    order = [(a, l, 2, j) for a, l in Z_FIRST for j in (0, 1)]
    order += [(a, l, 2, 1) for a, l in Y_FIRST]
    order += [(a, l, down(l), j) for a, l in Z_FIRST for j in (0, 1)]
    order += [(a, l, k, 1) for k in (1, 3) for a, l in Y_FIRST]
    order += [(a, l, up(l), j) for a, l in Z_FIRST for j in (0, 1)]
    order += [(a, l, 0, 1) for a, l in Y_FIRST]
    order += [(a, l, 2, 0) for a, l in Y_FIRST]
    order += [(a, l, k, 0) for k in (1, 3) for a, l in Y_FIRST]
    order += [(a, l, 0, j) for a, l in Z_FIRST for j in (0, 1)]
    order += [(a, l, 0, 0) for a, l in Y_FIRST]

    loaded, from_peer = {}, {}
    for a, l, k, j in order:
        loaded[a, l, k, j] = load(block(delta, a, l, ys[j], zs[k], c), own[a].at[l, k, j])
    state = []
    for a in range(3):
        state.append(load(master[a], held_master[a]))
        state.append(load(moment[a], held_moment[a]))

    barrier = pltpu.get_barrier_semaphore()
    for to in (core_to, {"z": zs[1]}, {"z": zs[3]}, y_to):
        pl.semaphore_signal(barrier, inc=1, device_id=to, device_id_type=MESH)
    pl.semaphore_wait(barrier, 4)

    for a, l, k, j in order:
        from_peer[a, l, k, j] = send(
            block(delta, a, l, ys[j], zs[k], 1 - c), peer[a].at[l, k, j], core_to
        )

    def pair(a, l, k, j):
        loaded[a, l, k, j].wait()
        from_peer[a, l, k, j].wait_recv()
        own[a][l, k, j] = own[a][l, k, j] + peer[a][l, k, j]

    got = {}
    for a, l in Z_FIRST:
        pair(a, l, 2, 0)
        pair(a, l, 2, 1)
    for a, l in Z_FIRST:
        got["far", a, l] = send(own[a].at[l, 2], far[a].at[l], {"z": zs[up(l)]})
    for a, l in Y_FIRST:
        pair(a, l, 2, 1)
    for a, l in Y_FIRST:
        got["y", a, l, 2] = send(own[a].at[l, 2, 1], across[a].at[l, 2], y_to)
    for a, l in Z_FIRST:
        pair(a, l, down(l), 0)
        pair(a, l, down(l), 1)
    for a, l in Z_FIRST:
        got["direct", a, l] = send(own[a].at[l, down(l)], direct[a].at[l], {"z": zs[down(l)]})
    for k in (1, 3):
        for a, l in Y_FIRST:
            pair(a, l, k, 1)
        for a, l in Y_FIRST:
            got["y", a, l, k] = send(own[a].at[l, k, 1], across[a].at[l, k], y_to)
    for a, l in Z_FIRST:
        pair(a, l, up(l), 0)
        pair(a, l, up(l), 1)
    for a, l in Y_FIRST:
        pair(a, l, 0, 1)
    for a, l in Y_FIRST:
        got["y", a, l, 0] = send(own[a].at[l, 0, 1], across[a].at[l, 0], y_to)
    for k in (2, 1, 3):
        for a, l in Y_FIRST:
            pair(a, l, k, 0)
    for a, l in Z_FIRST:
        pair(a, l, 0, 0)
        pair(a, l, 0, 1)
    for a, l in Y_FIRST:
        pair(a, l, 0, 0)

    for a, l in Z_FIRST:
        got["far", a, l].wait_recv()
        own[a][l, up(l)] = (
            own[a][l, up(l)].astype(f32) + far[a][l].astype(f32)
        ).astype(bf16)
        got["summed", a, l] = send(own[a].at[l, up(l)], summed[a].at[l], {"z": zs[up(l)]})
    for a, l in Y_FIRST:
        got["y", a, l, 2].wait_recv()
        own[a][l, 2, 0] = own[a][l, 2, 0] + across[a][l, 2]
        got["far", a, l] = send(own[a].at[l, 2, 0], far[a].at[l, 0], {"z": zs[up(l)]})
    for k in (1, 3):
        for a, l in Y_FIRST:
            got["y", a, l, k].wait_recv()
            if k == down(l):
                own[a][l, k, 0] = own[a][l, k, 0] + across[a][l, k]
                got["direct", a, l] = send(
                    own[a].at[l, k, 0], direct[a].at[l, 0], {"z": zs[k]}
                )
    total = {}
    for a, l in Z_FIRST:
        got["direct", a, l].wait_recv()
        got["summed", a, l].wait_recv()
        mine = [
            own[a][l, 0, j].astype(f32) + direct[a][l, j].astype(f32) + summed[a][l, j].astype(f32)
            for j in (0, 1)
        ]
        own[a][l, 0, 1] = mine[1].astype(bf16)
        got["y", a, l, 0] = send(own[a].at[l, 0, 1], across[a].at[l, 0], y_to)
    for a, l in Y_FIRST:
        got["far", a, l].wait_recv()
        k = up(l)
        own[a][l, k, 0] = (
            own[a][l, k, 0].astype(f32)
            + across[a][l, k].astype(f32)
            + far[a][l, 0].astype(f32)
        ).astype(bf16)
        got["summed", a, l] = send(own[a].at[l, k, 0], summed[a].at[l, 0], {"z": zs[k]})

    for copy in state:
        copy.wait()

    def update(a, l):
        pieces = [own[a][l, 0, 0], direct[a][l, 0], summed[a][l, 0], across[a][l, 0]]
        average = sum(piece.astype(f32) for piece in pieces) * (1.0 / REPLICAS)
        momentum = OUTER_MOMENTUM * held_moment[a][l] + average
        updated = held_master[a][l] - OUTER_RATE * (average + OUTER_MOMENTUM * momentum)
        new_moment[a][l] = momentum
        new_master[a][l] = updated
        block(params, a, l, yh, z, c)[...] = updated.astype(bf16)

    def share(a, l, y, zz, to):
        piece = block(params, a, l, y, zz, c)
        return send(piece, piece, to)

    to_core = []

    def core_share(a, l, y, k):
        to_core.append(share(a, l, y, zs[k], core_to))

    for a, l in Y_FIRST:
        got["y", a, l, 0].wait_recv()
        got["direct", a, l].wait_recv()
        got["summed", a, l].wait_recv()
        update(a, l)
    up_copy, down_copy, on_copy, y_copy = {}, {}, {}, {}

    def z_share(a, l, j):
        up_copy[a, l, j] = share(a, l, ys[j], z, {"z": zs[up(l)]})

    def z_share_back(a, l, j):
        down_copy[a, l, j] = share(a, l, ys[j], z, {"z": zs[down(l)]})

    for a, l in Y_FIRST:
        z_share(a, l, 0)
    for a, l in Y_FIRST:
        y_copy[a, l, 0] = share(a, l, yh, z, y_to)
    for a, l in Y_FIRST:
        z_share_back(a, l, 0)
    for a, l in Y_FIRST:
        core_share(a, l, yh, 0)

    for a, l in Z_FIRST:
        got["y", a, l, 0].wait_recv()
        update(a, l)
    for a, l in Z_FIRST:
        y_copy[a, l, 0] = share(a, l, yh, z, y_to)
    for a, l in Z_FIRST:
        core_share(a, l, yh, 0)
    for a, l in Y_FIRST:
        up_copy[a, l, 0].wait_recv()
        on_copy[a, l, 0] = share(a, l, yh, zs[down(l)], {"z": zs[up(l)]})
    for a, l in Z_FIRST:
        z_share(a, l, 0)
    for a, l in Z_FIRST:
        z_share_back(a, l, 0)
    for a, l in Y_FIRST:
        y_copy[a, l, down(l)] = share(a, l, yh, zs[down(l)], y_to)
        core_share(a, l, yh, down(l))
    for a, l in Y_FIRST:
        down_copy[a, l, 0].wait_recv()
        y_copy[a, l, up(l)] = share(a, l, yh, zs[up(l)], y_to)
        core_share(a, l, yh, up(l))
    for a, l in Y_FIRST:
        on_copy[a, l, 0].wait_recv()
        y_copy[a, l, 2] = share(a, l, yh, zs[2], y_to)
        core_share(a, l, yh, 2)
    for a, l in Y_FIRST:
        y_copy[a, l, 0].wait_recv()
        core_share(a, l, ys[1], 0)
    for a, l in Z_FIRST:
        y_copy[a, l, 0].wait_recv()
        z_share(a, l, 1)
    for a, l in Z_FIRST:
        up_copy[a, l, 0].wait_recv()
        on_copy[a, l, 0] = share(a, l, yh, zs[down(l)], {"z": zs[up(l)]})
    for a, l in Z_FIRST:
        z_share_back(a, l, 1)
        core_share(a, l, ys[1], 0)
        core_share(a, l, yh, down(l))
    for a, l in Z_FIRST:
        down_copy[a, l, 0].wait_recv()
        core_share(a, l, yh, up(l))
    for k in (1, 3):
        for a, l in Y_FIRST:
            if k == down(l):
                y_copy[a, l, k].wait_recv()
                core_share(a, l, ys[1], k)
    for a, l in Z_FIRST:
        on_copy[a, l, 0].wait_recv()
        core_share(a, l, yh, 2)
    for a, l in Z_FIRST:
        up_copy[a, l, 1].wait_recv()
        on_copy[a, l, 1] = share(a, l, ys[1], zs[down(l)], {"z": zs[up(l)]})
        core_share(a, l, ys[1], down(l))
    for a, l in Z_FIRST:
        down_copy[a, l, 1].wait_recv()
        core_share(a, l, ys[1], up(l))
    for k in (1, 3):
        for a, l in Y_FIRST:
            if k == up(l):
                y_copy[a, l, k].wait_recv()
                core_share(a, l, ys[1], k)
    for a, l in Z_FIRST:
        on_copy[a, l, 1].wait_recv()
        core_share(a, l, ys[1], 2)
    for a, l in Y_FIRST:
        y_copy[a, l, 2].wait_recv()
        core_share(a, l, ys[1], 2)
    for copy in to_core:
        copy.wait_recv()
    for copy in started:
        copy.wait_send()


def outer_step(
    delta_query,
    master_query,
    moment_query,
    delta_latent,
    master_latent,
    moment_latent,
    delta_output,
    master_output,
    moment_output,
):
    f32, bf16 = jnp.float32, jnp.bfloat16
    shapes = []
    for a, block in enumerate(BLOCKS):
        whole = (LAYERS, 2, 4, 2, *block) if a < 2 else (LAYERS, block[0], 16 * block[1])
        shapes += [(whole, bf16), ((LAYERS, *block), f32), ((LAYERS, *block), f32)]
    pieces = [(LAYERS, 4, 2), (LAYERS, 4, 2), (LAYERS, 2), (LAYERS, 2), (LAYERS, 2), (LAYERS, 4)]
    scratch = [pltpu.VMEM((*lead, *block), bf16) for lead in pieces for block in BLOCKS]
    scratch += [pltpu.VMEM((LAYERS, *block), f32) for _ in range(2) for block in BLOCKS]
    results = pl.pallas_call(
        outer_kernel,
        out_shape=tuple(pltpu.VMEM(*shape) for shape in shapes),
        in_specs=[pl.BlockSpec(memory_space=pl.ANY)] * 9,
        out_specs=tuple(pl.BlockSpec(memory_space=pltpu.VMEM) for _ in range(9)),
        scratch_shapes=scratch
        + [
            pltpu.SemaphoreType.DMA((LOADS,)),
            pltpu.SemaphoreType.DMA((COPIES,)),
            pltpu.SemaphoreType.DMA((COPIES,)),
        ],
        compiler_params=pltpu.CompilerParams(
            collective_id=0, has_side_effects=True, vmem_limit_bytes=40 * 1024 * 1024
        ),
    )(
        delta_query.reshape(shapes[0][0]),
        master_query,
        moment_query,
        delta_latent.reshape(shapes[3][0]),
        master_latent,
        moment_latent,
        delta_output.reshape(shapes[6][0]),
        master_output,
        moment_output,
    )
    query, latent = results[0], results[3]
    return (
        query.reshape(LAYERS, 2048, 384),
        *results[1:3],
        latent.reshape(LAYERS, 512, 512),
        *results[4:],
    )


def solution(mesh):
    torus = Mesh(mesh.devices.reshape(2, 4, 2, 2, 4), (*REP, *TP))
    return jax.shard_map(
        outer_step,
        mesh=torus,
        in_specs=(
            P(REP, None, None, TP),
            P(None, REP, TP),
            P(None, REP, TP),
            P(REP, None, None, TP),
            P(None, REP, TP),
            P(None, REP, TP),
            P(REP, None, TP, None),
            P(None, TP, REP),
            P(None, TP, REP),
        ),
        out_specs=(
            P(None, None, TP),
            P(None, REP, TP),
            P(None, REP, TP),
            P(None, None, TP),
            P(None, REP, TP),
            P(None, REP, TP),
            P(None, TP, None),
            P(None, TP, REP),
            P(None, TP, REP),
        ),
        check_vma=False,
    )
```

```python
import jax
import jax.numpy as jnp
from jax import lax
from jax.experimental import pallas as pl
from jax.experimental.pallas import tpu as pltpu
from jax.sharding import Mesh
from jax.sharding import PartitionSpec as P

REP = ("yh", "z", "c")
TP = ("yl", "x")
MESH = pl.DeviceIdType.MESH

OUTER_RATE = 0.7
OUTER_MOMENTUM = 0.9
REPLICAS = 16

BLOCKS = ((128, 384), (32, 512), (256, 128))
LAYERS = 2
Z_FIRST = ((0, 0), (0, 1))
Y_FIRST = ((1, 0), (1, 1), (2, 0), (2, 1))
COPIES = 256
LOADS = 64


def outer_kernel(*refs):
    f32, bf16 = jnp.float32, jnp.bfloat16
    delta, master, moment = refs[0:9:3], refs[1:9:3], refs[2:9:3]
    params, new_master, new_moment = refs[9:18:3], refs[10:18:3], refs[11:18:3]
    own, peer, far, direct, summed, across, held_master, held_moment = (
        refs[18 + 3 * i : 21 + 3 * i] for i in range(8)
    )
    load_sem, send_sem, recv_sem = refs[42:]

    yh, z, c = (lax.axis_index(a) for a in REP)
    zs = [lax.rem(z + k, 4) for k in range(4)]
    ys = [yh, 1 - yh]
    core_to, y_to = {"c": 1 - c}, {"yh": 1 - yh}

    def up(layer):
        return 1 if layer == 0 else 3

    def down(layer):
        return 3 if layer == 0 else 1

    started, loads = [], []

    def send(src, dst, to):
        i = len(started)
        copy = pltpu.make_async_remote_copy(
            src_ref=src,
            dst_ref=dst,
            send_sem=send_sem.at[i],
            recv_sem=recv_sem.at[i],
            device_id=to,
            device_id_type=MESH,
        )
        copy.start()
        started.append(copy)
        return copy

    def load(src, dst):
        copy = pltpu.make_async_copy(src, dst, load_sem.at[len(loads)])
        copy.start()
        loads.append(copy)
        return copy

    def block(ref, a, layer, y, zz, core):
        if a < 2:
            return ref[a].at[layer, y, zz, core]
        column = pl.multiple_of(((y * 4 + zz) * 2 + core) * 128, 128)
        return ref[2].at[layer, :, pl.ds(column, 128)]

    order = [(a, l, 2, j) for a, l in Z_FIRST for j in (0, 1)]
    order += [(a, l, 2, 1) for a, l in Y_FIRST]
    order += [(a, l, down(l), j) for a, l in Z_FIRST for j in (0, 1)]
    order += [(a, l, k, 1) for k in (1, 3) for a, l in Y_FIRST]
    order += [(a, l, up(l), j) for a, l in Z_FIRST for j in (0, 1)]
    order += [(a, l, 0, 1) for a, l in Y_FIRST]
    order += [(a, l, 2, 0) for a, l in Y_FIRST]
    order += [(a, l, k, 0) for k in (1, 3) for a, l in Y_FIRST]
    order += [(a, l, 0, j) for a, l in Z_FIRST for j in (0, 1)]
    order += [(a, l, 0, 0) for a, l in Y_FIRST]

    loaded, from_peer = {}, {}
    for a, l, k, j in order:
        loaded[a, l, k, j] = load(block(delta, a, l, ys[j], zs[k], c), own[a].at[l, k, j])
    state = []
    for a in range(3):
        state.append(load(master[a], held_master[a]))
        state.append(load(moment[a], held_moment[a]))

    barrier = pltpu.get_barrier_semaphore()
    for to in (core_to, {"z": zs[1]}, {"z": zs[3]}, y_to):
        pl.semaphore_signal(barrier, inc=1, device_id=to, device_id_type=MESH)
    pl.semaphore_wait(barrier, 4)

    for a, l, k, j in order:
        from_peer[a, l, k, j] = send(
            block(delta, a, l, ys[j], zs[k], 1 - c), peer[a].at[l, k, j], core_to
        )

    def pair(a, l, k, j):
        loaded[a, l, k, j].wait()
        from_peer[a, l, k, j].wait_recv()
        own[a][l, k, j] = own[a][l, k, j] + peer[a][l, k, j]

    got = {}
    for a, l in Z_FIRST:
        pair(a, l, 2, 0)
        pair(a, l, 2, 1)
    for a, l in Z_FIRST:
        got["far", a, l] = send(own[a].at[l, 2], far[a].at[l], {"z": zs[up(l)]})
    for a, l in Y_FIRST:
        pair(a, l, 2, 1)
    for a, l in Y_FIRST:
        got["y", a, l, 2] = send(own[a].at[l, 2, 1], across[a].at[l, 2], y_to)
    for a, l in Z_FIRST:
        pair(a, l, down(l), 0)
        pair(a, l, down(l), 1)
    for a, l in Z_FIRST:
        got["direct", a, l] = send(own[a].at[l, down(l)], direct[a].at[l], {"z": zs[down(l)]})
    for k in (1, 3):
        for a, l in Y_FIRST:
            pair(a, l, k, 1)
        for a, l in Y_FIRST:
            got["y", a, l, k] = send(own[a].at[l, k, 1], across[a].at[l, k], y_to)
    for a, l in Z_FIRST:
        pair(a, l, up(l), 0)
        pair(a, l, up(l), 1)
    for a, l in Y_FIRST:
        pair(a, l, 0, 1)
    for a, l in Y_FIRST:
        got["y", a, l, 0] = send(own[a].at[l, 0, 1], across[a].at[l, 0], y_to)
    for k in (2, 1, 3):
        for a, l in Y_FIRST:
            pair(a, l, k, 0)
    for a, l in Z_FIRST:
        pair(a, l, 0, 0)
        pair(a, l, 0, 1)
    for a, l in Y_FIRST:
        pair(a, l, 0, 0)

    for a, l in Z_FIRST:
        got["far", a, l].wait_recv()
        own[a][l, up(l)] = (
            own[a][l, up(l)].astype(f32) + far[a][l].astype(f32)
        ).astype(bf16)
        got["summed", a, l] = send(own[a].at[l, up(l)], summed[a].at[l], {"z": zs[up(l)]})
    for a, l in Y_FIRST:
        got["y", a, l, 2].wait_recv()
        own[a][l, 2, 0] = own[a][l, 2, 0] + across[a][l, 2]
        got["far", a, l] = send(own[a].at[l, 2, 0], far[a].at[l, 0], {"z": zs[up(l)]})
    for k in (1, 3):
        for a, l in Y_FIRST:
            got["y", a, l, k].wait_recv()
            if k == down(l):
                own[a][l, k, 0] = own[a][l, k, 0] + across[a][l, k]
                got["direct", a, l] = send(
                    own[a].at[l, k, 0], direct[a].at[l, 0], {"z": zs[k]}
                )
    total = {}
    for a, l in Z_FIRST:
        got["direct", a, l].wait_recv()
        got["summed", a, l].wait_recv()
        mine = [
            own[a][l, 0, j].astype(f32) + direct[a][l, j].astype(f32) + summed[a][l, j].astype(f32)
            for j in (0, 1)
        ]
        own[a][l, 0, 1] = mine[1].astype(bf16)
        got["y", a, l, 0] = send(own[a].at[l, 0, 1], across[a].at[l, 0], y_to)
    for a, l in Y_FIRST:
        got["far", a, l].wait_recv()
        k = up(l)
        own[a][l, k, 0] = (
            own[a][l, k, 0].astype(f32)
            + across[a][l, k].astype(f32)
            + far[a][l, 0].astype(f32)
        ).astype(bf16)
        got["summed", a, l] = send(own[a].at[l, k, 0], summed[a].at[l, 0], {"z": zs[k]})

    for copy in state:
        copy.wait()

    def update(a, l):
        pieces = [own[a][l, 0, 0], direct[a][l, 0], summed[a][l, 0], across[a][l, 0]]
        average = sum(piece.astype(f32) for piece in pieces) * (1.0 / REPLICAS)
        momentum = OUTER_MOMENTUM * held_moment[a][l] + average
        updated = held_master[a][l] - OUTER_RATE * (average + OUTER_MOMENTUM * momentum)
        new_moment[a][l] = momentum
        new_master[a][l] = updated
        block(params, a, l, yh, z, c)[...] = updated.astype(bf16)

    def share(a, l, y, zz, to):
        piece = block(params, a, l, y, zz, c)
        return send(piece, piece, to)

    to_core = []

    def core_share(a, l, y, k):
        to_core.append(share(a, l, y, zs[k], core_to))

    for a, l in Y_FIRST:
        got["y", a, l, 0].wait_recv()
        got["direct", a, l].wait_recv()
        got["summed", a, l].wait_recv()
        update(a, l)
    up_copy, down_copy, on_copy, y_copy = {}, {}, {}, {}

    def z_share(a, l, j):
        up_copy[a, l, j] = share(a, l, ys[j], z, {"z": zs[up(l)]})

    def z_share_back(a, l, j):
        down_copy[a, l, j] = share(a, l, ys[j], z, {"z": zs[down(l)]})

    for a, l in Y_FIRST:
        z_share(a, l, 0)
    for a, l in Y_FIRST:
        y_copy[a, l, 0] = share(a, l, yh, z, y_to)
    for a, l in Y_FIRST:
        z_share_back(a, l, 0)
    for a, l in Y_FIRST:
        core_share(a, l, yh, 0)

    for a, l in Z_FIRST:
        got["y", a, l, 0].wait_recv()
        update(a, l)
    for a, l in Z_FIRST:
        y_copy[a, l, 0] = share(a, l, yh, z, y_to)
    for a, l in Z_FIRST:
        core_share(a, l, yh, 0)
    for a, l in Y_FIRST:
        up_copy[a, l, 0].wait_recv()
        on_copy[a, l, 0] = share(a, l, yh, zs[down(l)], {"z": zs[up(l)]})
    for a, l in Z_FIRST:
        z_share(a, l, 0)
    for a, l in Z_FIRST:
        z_share_back(a, l, 0)
    for a, l in Y_FIRST:
        y_copy[a, l, down(l)] = share(a, l, yh, zs[down(l)], y_to)
        core_share(a, l, yh, down(l))
    for a, l in Y_FIRST:
        down_copy[a, l, 0].wait_recv()
        y_copy[a, l, up(l)] = share(a, l, yh, zs[up(l)], y_to)
        core_share(a, l, yh, up(l))
    for a, l in Y_FIRST:
        on_copy[a, l, 0].wait_recv()
        y_copy[a, l, 2] = share(a, l, yh, zs[2], y_to)
        core_share(a, l, yh, 2)
    for a, l in Y_FIRST:
        y_copy[a, l, 0].wait_recv()
        core_share(a, l, ys[1], 0)
    for a, l in Z_FIRST:
        y_copy[a, l, 0].wait_recv()
        z_share(a, l, 1)
    for a, l in Z_FIRST:
        up_copy[a, l, 0].wait_recv()
        on_copy[a, l, 0] = share(a, l, yh, zs[down(l)], {"z": zs[up(l)]})
    for a, l in Z_FIRST:
        z_share_back(a, l, 1)
        core_share(a, l, ys[1], 0)
        core_share(a, l, yh, down(l))
    for a, l in Z_FIRST:
        down_copy[a, l, 0].wait_recv()
        core_share(a, l, yh, up(l))
    for k in (1, 3):
        for a, l in Y_FIRST:
            if k == down(l):
                y_copy[a, l, k].wait_recv()
                core_share(a, l, ys[1], k)
    for a, l in Z_FIRST:
        on_copy[a, l, 0].wait_recv()
        core_share(a, l, yh, 2)
    for a, l in Z_FIRST:
        up_copy[a, l, 1].wait_recv()
        on_copy[a, l, 1] = share(a, l, ys[1], zs[down(l)], {"z": zs[up(l)]})
        core_share(a, l, ys[1], down(l))
    for a, l in Z_FIRST:
        down_copy[a, l, 1].wait_recv()
        core_share(a, l, ys[1], up(l))
    for k in (1, 3):
        for a, l in Y_FIRST:
            if k == up(l):
                y_copy[a, l, k].wait_recv()
                core_share(a, l, ys[1], k)
    for a, l in Z_FIRST:
        on_copy[a, l, 1].wait_recv()
        core_share(a, l, ys[1], 2)
    for a, l in Y_FIRST:
        y_copy[a, l, 2].wait_recv()
        core_share(a, l, ys[1], 2)
    for copy in to_core:
        copy.wait_recv()
    for copy in started:
        copy.wait_send()


def write_kernel(*refs):
    sources, results, sem = refs[:9], refs[9:18], refs[18]
    copies = []
    for source, result in zip(sources, results):
        for layer in range(LAYERS):
            copies.append(
                pltpu.make_async_copy(source.at[layer], result.at[layer], sem.at[len(copies)])
            )
    for copy in copies:
        copy.start()
    for copy in copies:
        copy.wait()


def outer_step(
    delta_query,
    master_query,
    moment_query,
    delta_latent,
    master_latent,
    moment_latent,
    delta_output,
    master_output,
    moment_output,
):
    f32, bf16 = jnp.float32, jnp.bfloat16
    shapes = []
    for a, block in enumerate(BLOCKS):
        whole = (LAYERS, 2, 4, 2, *block) if a < 2 else (LAYERS, block[0], 16 * block[1])
        shapes += [(whole, bf16), ((LAYERS, *block), f32), ((LAYERS, *block), f32)]
    pieces = [(LAYERS, 4, 2), (LAYERS, 4, 2), (LAYERS, 2), (LAYERS, 2), (LAYERS, 2), (LAYERS, 4)]
    scratch = [pltpu.VMEM((*lead, *block), bf16) for lead in pieces for block in BLOCKS]
    scratch += [pltpu.VMEM((LAYERS, *block), f32) for _ in range(2) for block in BLOCKS]
    operands = (
        delta_query.reshape(shapes[0][0]),
        master_query,
        moment_query,
        delta_latent.reshape(shapes[3][0]),
        master_latent,
        moment_latent,
        delta_output.reshape(shapes[6][0]),
        master_output,
        moment_output,
    )
    operands = [pltpu.with_memory_space_constraint(x, pltpu.HBM) for x in operands]
    results = pl.pallas_call(
        outer_kernel,
        out_shape=tuple(pltpu.VMEM(*shape) for shape in shapes),
        in_specs=[pl.BlockSpec(memory_space=pltpu.HBM)] * 9,
        out_specs=tuple(pl.BlockSpec(memory_space=pltpu.VMEM) for _ in range(9)),
        scratch_shapes=scratch
        + [
            pltpu.SemaphoreType.DMA((LOADS,)),
            pltpu.SemaphoreType.DMA((COPIES,)),
            pltpu.SemaphoreType.DMA((COPIES,)),
        ],
        compiler_params=pltpu.CompilerParams(
            collective_id=0, has_side_effects=True, vmem_limit_bytes=40 * 1024 * 1024
        ),
    )(*operands)
    results = [pltpu.with_memory_space_constraint(x, pltpu.VMEM) for x in results]
    results = pl.pallas_call(
        write_kernel,
        out_shape=tuple(pltpu.HBM(*shape) for shape in shapes),
        in_specs=[pl.BlockSpec(memory_space=pltpu.VMEM)] * 9,
        out_specs=tuple(pl.BlockSpec(memory_space=pltpu.HBM) for _ in range(9)),
        scratch_shapes=[pltpu.SemaphoreType.DMA((9 * LAYERS,))],
        compiler_params=pltpu.CompilerParams(vmem_limit_bytes=4 * 1024 * 1024),
    )(*results)
    query, latent = results[0], results[3]
    return (
        query.reshape(LAYERS, 2048, 384),
        *results[1:3],
        latent.reshape(LAYERS, 512, 512),
        *results[4:],
    )


def solution(mesh):
    torus = Mesh(mesh.devices.reshape(2, 4, 2, 2, 4), (*REP, *TP))
    return jax.shard_map(
        outer_step,
        mesh=torus,
        in_specs=(
            P(REP, None, None, TP),
            P(None, REP, TP),
            P(None, REP, TP),
            P(REP, None, None, TP),
            P(None, REP, TP),
            P(None, REP, TP),
            P(REP, None, TP, None),
            P(None, TP, REP),
            P(None, TP, REP),
        ),
        out_specs=(
            P(None, None, TP),
            P(None, REP, TP),
            P(None, REP, TP),
            P(None, None, TP),
            P(None, REP, TP),
            P(None, REP, TP),
            P(None, TP, None),
            P(None, TP, REP),
            P(None, TP, REP),
        ),
        check_vma=False,
    )
```

```python
import math

import jax
import jax.numpy as jnp
from jax import lax
from jax.experimental import pallas as pl
from jax.experimental.pallas import tpu as pltpu
from jax.sharding import Mesh
from jax.sharding import PartitionSpec as P

REP = ("yh", "z", "c")
TP = ("yl", "x")
MESH = pl.DeviceIdType.MESH

OUTER_RATE = 0.7
OUTER_MOMENTUM = 0.9
REPLICAS = 16
LAYERS = 2

BLOCKS = ((128, 384), (32, 512), (256, 128))
PARTS = ((0, 0, 64), (0, 64, 64), (1, 0, 16), (1, 16, 16), (2, 0, 256))
A, B, C = (0,), (1, 2), (3, 4)
Z_FIRST, Y_FIRST = (A, B), (C,)
GROUPS = 56
SENDS = 4
LOADS = 4
SIZE_ROWS = 3 * 4096


def part_shape(p):
    array, _, rows = PARTS[p]
    return (rows, BLOCKS[array][1])


def outer_kernel(*refs):
    f32, bf16 = jnp.float32, jnp.bfloat16
    delta, master, moment = refs[0:9:3], refs[1:9:3], refs[2:9:3]
    params, new_master, new_moment = refs[9:18:3], refs[10:18:3], refs[11:18:3]
    n = len(PARTS)
    own, peer, far, direct, summed, across = (
        refs[18 + n * i : 18 + n * (i + 1)] for i in range(6)
    )
    rest = refs[18 + 6 * n :]
    held_master, held_moment = rest[0:3], rest[3:6]
    size, load_sem, send_sem, recv_sem = rest[6:]

    yh, z, c = (lax.axis_index(a) for a in REP)
    zs = [lax.rem(z + k, 4) for k in range(4)]
    ys = [yh, 1 - yh]
    core_to, y_to = {"c": 1 - c}, {"yh": 1 - yh}
    z_to = {1: {"z": zs[1]}, 3: {"z": zs[3]}}
    up, down = (1, 3), (3, 1)

    barrier = pltpu.get_barrier_semaphore()
    for to in (y_to, z_to[1], z_to[3], core_to):
        pl.semaphore_signal(barrier, inc=1, device_id=to, device_id_type=MESH)

    def wait_bytes(sem, total):
        piece = size.at[pl.ds(0, total // 256)]
        pltpu.make_async_remote_copy(
            src_ref=piece,
            dst_ref=piece,
            send_sem=sem,
            recv_sem=sem,
            device_id=core_to,
            device_id_type=MESH,
        ).wait_recv()

    groups, sent, load_bytes = {}, [0] * SENDS, [0] * LOADS

    def send(src, dst, to, group, which):
        index, total = groups.get(group, (len(groups), 0))
        count = 2 * math.prod(src.shape)
        groups[group] = (index, total + count)
        sent[which] += count
        pltpu.make_async_remote_copy(
            src_ref=src,
            dst_ref=dst,
            send_sem=send_sem.at[which],
            recv_sem=recv_sem.at[index],
            device_id=to,
            device_id_type=MESH,
        ).start()

    def arrive(*group):
        index, total = groups[group]
        wait_bytes(recv_sem.at[index], total)

    def load(src, dst, which, width):
        load_bytes[which] += width * math.prod(src.shape)
        pltpu.make_async_copy(src, dst, load_sem.at[which]).start()

    def block(ref, p, layer, y, zz, core):
        array, first, rows = PARTS[p]
        if array < 2:
            return ref[array].at[layer, y, zz, core, pl.ds(first, rows)]
        column = pl.multiple_of(((y * 4 + zz) * 2 + core) * 128, 128)
        return ref[2].at[layer, pl.ds(first, rows), pl.ds(column, 128)]

    both = slice(None)

    order = (
        (A, (2,), (0, 1), 0),
        (C, (2,), (1,), 1),
        (A, (1, 3), (0, 1), 2),
        (C, (1, 3), (1,), 2),
        (B, (2,), (0, 1), 2),
        (C, (0,), (1,), 2),
        (B, (1, 3), (0, 1), 2),
        (A, (0,), (0, 1), 2),
        (C, (2, 1, 3), (0,), 2),
        (B, (0,), (0, 1), 2),
        (C, (0,), (0,), 2),
    )
    for chunk, ks, js, which in order:
        for p in chunk:
            for k in ks:
                for j in js:
                    load(block(delta, p, both, ys[j], zs[k], c), own[p].at[:, k, j], which, 2)
    for a in range(3):
        load(master[a], held_master[a], 3, 4)
        load(moment[a], held_moment[a], 3, 4)

    pl.semaphore_wait(barrier, 4)

    for chunk, ks, js, which in order:
        for p in chunk:
            for k in ks:
                for j in js:
                    send(
                        block(delta, p, both, ys[j], zs[k], 1 - c),
                        peer[p].at[:, k, j],
                        core_to,
                        ("core", chunk, ks, js),
                        0,
                    )

    waited = set()

    def pair(step):
        chunk, ks, js, which = order[step]
        if which not in waited:
            waited.add(which)
            wait_bytes(load_sem.at[which], load_bytes[which])
        arrive("core", chunk, ks, js)
        for p in chunk:
            for k in ks:
                for j in js:
                    own[p][:, k, j] = own[p][:, k, j] + peer[p][:, k, j]

    def total_of(*pieces):
        return sum(piece.astype(f32) for piece in pieces)

    layers = range(LAYERS)

    def zy_far(chunk):
        for l in layers:
            for p in chunk:
                send(own[p].at[l, 2], far[p].at[l], z_to[up[l]], ("far", chunk), 1)

    def zy_direct(chunk):
        for l in layers:
            for p in chunk:
                k = down[l]
                send(own[p].at[l, k], direct[p].at[l], z_to[k], ("direct", chunk), 1)

    def zy_pass_on(chunk):
        arrive("far", chunk)
        for l in layers:
            for p in chunk:
                k = up[l]
                own[p][l, k] = total_of(own[p][l, k], far[p][l]).astype(bf16)
                send(own[p].at[l, k], summed[p].at[l], z_to[k], ("summed", chunk), 1)

    def zy_across(chunk):
        arrive("direct", chunk)
        arrive("summed", chunk)
        for p in chunk:
            for l in layers:
                own[p][l, 0, 1] = total_of(
                    own[p][l, 0, 1], direct[p][l, 1], summed[p][l, 1]
                ).astype(bf16)
            send(own[p].at[:, 0, 1], across[p].at[:, 0], y_to, ("y", chunk), 1)

    def yz_across(chunk, k):
        for p in chunk:
            send(own[p].at[:, k, 1], across[p].at[:, k], y_to, ("y", chunk, k), 1)

    def yz_far(chunk):
        arrive("y", chunk, 2)
        for l in layers:
            for p in chunk:
                own[p][l, 2, 0] = own[p][l, 2, 0] + across[p][l, 2]
                send(own[p].at[l, 2, 0], far[p].at[l, 0], z_to[up[l]], ("far", chunk), 1)

    def yz_direct(chunk):
        arrive("y", chunk, 1)
        arrive("y", chunk, 3)
        for l in layers:
            for p in chunk:
                k = down[l]
                own[p][l, k, 0] = own[p][l, k, 0] + across[p][l, k]
                send(own[p].at[l, k, 0], direct[p].at[l, 0], z_to[k], ("direct", chunk), 1)

    def yz_pass_on(chunk):
        arrive("far", chunk)
        for l in layers:
            for p in chunk:
                k = up[l]
                own[p][l, k, 0] = total_of(own[p][l, k, 0], across[p][l, k], far[p][l, 0]).astype(
                    bf16
                )
                send(own[p].at[l, k, 0], summed[p].at[l, 0], z_to[k], ("summed", chunk), 1)

    def update(chunk):
        for p in chunk:
            a, first, rows = PARTS[p]
            for l in layers:
                here = (l, pl.ds(first, rows))
                total = total_of(own[p][l, 0, 0], direct[p][l, 0], summed[p][l, 0], across[p][l, 0])
                average = total * (1.0 / REPLICAS)
                momentum = OUTER_MOMENTUM * held_moment[a][here] + average
                updated = held_master[a][here] - OUTER_RATE * (
                    average + OUTER_MOMENTUM * momentum
                )
                new_moment[a][here] = momentum
                new_master[a][here] = updated
                block(params, p, l, yh, z, c)[...] = updated.astype(bf16)

    def share(p, l, y, zz, to, group, which=2):
        piece = block(params, p, l, y, zz, c)
        send(piece, piece, to, group, which)

    def core_share(p, l, j, k):
        share(p, l, ys[j], zs[k], core_to, ("core",), 3)

    def gather_z(chunk, j):
        for name, way in (("up", up), ("down", down)):
            for l in layers:
                for p in chunk:
                    share(p, l, ys[j], z, z_to[way[l]], (name, chunk, j))

    def gather_own(chunk, j):
        for p in chunk:
            core_share(p, both, j, 0)

    def gather_y(chunk):
        for p in chunk:
            share(p, both, yh, z, y_to, ("across", chunk, "own"))

    def came(chunk, j, name):
        arrive(name, chunk, j)
        for l in layers:
            k = {"up": down[l], "down": up[l], "on": 2}[name]
            for p in chunk:
                if name == "up":
                    share(p, l, ys[j], zs[k], z_to[up[l]], ("on", chunk, j))
        for l in layers:
            k = {"up": down[l], "down": up[l], "on": 2}[name]
            for p in chunk:
                if chunk in Y_FIRST:
                    share(p, l, yh, zs[k], y_to, ("across", chunk, name))
                core_share(p, l, j, k)

    def came_across(chunk, name):
        arrive("across", chunk, name)
        for l in layers:
            k = {"own": 0, "up": down[l], "down": up[l], "on": 2}[name]
            for p in chunk:
                core_share(p, l, 1, k)

    pair(0)
    zy_far(A)
    pair(1)
    yz_across(C, 2)
    pair(2)
    zy_direct(A)
    pair(3)
    yz_across(C, 1)
    yz_across(C, 3)
    pair(4)
    zy_far(B)
    pair(5)
    yz_across(C, 0)
    pair(6)
    pair(7)
    pair(8)
    pair(9)
    pair(10)
    zy_pass_on(A)
    zy_direct(B)
    zy_pass_on(B)
    yz_far(C)
    zy_across(A)
    yz_direct(C)
    zy_across(B)
    yz_pass_on(C)
    wait_bytes(load_sem.at[3], load_bytes[3])
    arrive("y", A)
    update(A)
    gather_y(A)
    gather_z(A, 0)
    gather_own(A, 0)
    arrive("y", B)
    update(B)
    gather_y(B)
    arrive("y", C, 0)
    arrive("direct", C)
    arrive("summed", C)
    update(C)
    gather_z(C, 0)
    gather_y(C)
    gather_z(B, 0)
    gather_own(B, 0)
    gather_own(C, 0)
    came(A, 0, "up")
    came(A, 0, "down")
    came_across(A, "own")
    gather_z(A, 1)
    came(C, 0, "up")
    came(A, 0, "on")
    came(C, 0, "down")
    came_across(B, "own")
    gather_z(B, 1)
    came(C, 0, "on")
    came(B, 0, "up")
    came(B, 0, "down")
    came_across(C, "own")
    came(A, 1, "up")
    came(A, 1, "down")
    came_across(C, "up")
    came(B, 0, "on")
    came(B, 1, "up")
    came(A, 1, "on")
    came_across(C, "down")
    came(B, 1, "down")
    came(B, 1, "on")
    came_across(C, "on")
    arrive("core")
    for which in range(SENDS):
        wait_bytes(send_sem.at[which], sent[which])


def write_kernel(*refs):
    sources, results, sem = refs[:9], refs[9:18], refs[18]
    copies = []
    for source, result in zip(sources, results):
        for layer in range(LAYERS):
            copies.append(
                pltpu.make_async_copy(source.at[layer], result.at[layer], sem.at[len(copies)])
            )
    for copy in copies:
        copy.start()
    for copy in copies:
        copy.wait()


def outer_step(
    delta_query,
    master_query,
    moment_query,
    delta_latent,
    master_latent,
    moment_latent,
    delta_output,
    master_output,
    moment_output,
):
    f32, bf16 = jnp.float32, jnp.bfloat16
    shapes = []
    for a, block in enumerate(BLOCKS):
        whole = (LAYERS, 2, 4, 2, *block) if a < 2 else (LAYERS, block[0], 16 * block[1])
        shapes += [(whole, bf16), ((LAYERS, *block), f32), ((LAYERS, *block), f32)]
    z_first = {p for chunk in Z_FIRST for p in chunk}
    scratch = []
    for kind in range(6):
        for p in range(len(PARTS)):
            if kind < 2:
                lead = (LAYERS, 4, 2)
            elif kind < 5:
                lead = (LAYERS, 2 if p in z_first else 1)
            else:
                lead = (LAYERS, 1 if p in z_first else 4)
            scratch.append(pltpu.VMEM((*lead, *part_shape(p)), bf16))
    scratch += [pltpu.VMEM((LAYERS, *block), f32) for _ in range(2) for block in BLOCKS]
    operands = (
        delta_query.reshape(shapes[0][0]),
        master_query,
        moment_query,
        delta_latent.reshape(shapes[3][0]),
        master_latent,
        moment_latent,
        delta_output.reshape(shapes[6][0]),
        master_output,
        moment_output,
    )
    operands = [pltpu.with_memory_space_constraint(x, pltpu.HBM) for x in operands]
    results = pl.pallas_call(
        outer_kernel,
        out_shape=tuple(pltpu.VMEM(*shape) for shape in shapes),
        in_specs=[pl.BlockSpec(memory_space=pltpu.HBM)] * 9,
        out_specs=tuple(pl.BlockSpec(memory_space=pltpu.VMEM) for _ in range(9)),
        scratch_shapes=scratch
        + [
            pltpu.VMEM((SIZE_ROWS, 128), bf16),
            pltpu.SemaphoreType.DMA((LOADS,)),
            pltpu.SemaphoreType.DMA((SENDS,)),
            pltpu.SemaphoreType.DMA((GROUPS,)),
        ],
        compiler_params=pltpu.CompilerParams(
            collective_id=0, has_side_effects=True, vmem_limit_bytes=40 * 1024 * 1024
        ),
    )(*operands)
    results = [pltpu.with_memory_space_constraint(x, pltpu.VMEM) for x in results]
    results = pl.pallas_call(
        write_kernel,
        out_shape=tuple(pltpu.HBM(*shape) for shape in shapes),
        in_specs=[pl.BlockSpec(memory_space=pltpu.VMEM)] * 9,
        out_specs=tuple(pl.BlockSpec(memory_space=pltpu.HBM) for _ in range(9)),
        scratch_shapes=[pltpu.SemaphoreType.DMA((9 * LAYERS,))],
        compiler_params=pltpu.CompilerParams(vmem_limit_bytes=4 * 1024 * 1024),
    )(*results)
    query, latent = results[0], results[3]
    return (
        query.reshape(LAYERS, 2048, 384),
        *results[1:3],
        latent.reshape(LAYERS, 512, 512),
        *results[4:],
    )


def solution(mesh):
    torus = Mesh(mesh.devices.reshape(2, 4, 2, 2, 4), (*REP, *TP))
    return jax.shard_map(
        outer_step,
        mesh=torus,
        in_specs=(
            P(REP, None, None, TP),
            P(None, REP, TP),
            P(None, REP, TP),
            P(REP, None, None, TP),
            P(None, REP, TP),
            P(None, REP, TP),
            P(REP, None, TP, None),
            P(None, TP, REP),
            P(None, TP, REP),
        ),
        out_specs=(
            P(None, None, TP),
            P(None, REP, TP),
            P(None, REP, TP),
            P(None, None, TP),
            P(None, REP, TP),
            P(None, REP, TP),
            P(None, TP, None),
            P(None, TP, REP),
            P(None, TP, REP),
        ),
        check_vma=False,
    )
```

```python
import math

import jax
import jax.numpy as jnp
from jax import lax
from jax.experimental import pallas as pl
from jax.experimental.pallas import tpu as pltpu
from jax.sharding import Mesh
from jax.sharding import PartitionSpec as P

REP = ("yh", "z", "c")
TP = ("yl", "x")
MESH = pl.DeviceIdType.MESH

OUTER_RATE = 0.7
OUTER_MOMENTUM = 0.9
REPLICAS = 16
LAYERS = 2

BLOCKS = ((128, 384), (32, 512), (256, 128))
PARTS = ((0, 0, 64), (0, 64, 64), (1, 0, 16), (1, 16, 16), (2, 0, 256))
A, B, C = (0,), (1, 2), (3, 4)
Z_FIRST, Y_FIRST = (A, B), (C,)
GROUPS = 56
SENDS = 4
LOADS = 4
SIZE_ROWS = 3 * 4096


SCHEDULE = (
    ("pair", 0),
    ("zy_far", A),
    ("pair", 1),
    ("yz_across", C, 2),
    ("pair", 2),
    ("zy_direct", A),
    ("pair", 3),
    ("yz_across", C, 1),
    ("yz_across", C, 3),
    ("pair", 4),
    ("zy_far", B),
    ("pair", 5),
    ("yz_across", C, 0),
    ("pair", 6),
    ("pair", 7),
    ("pair", 8),
    ("pair", 9),
    ("pair", 10),
    ("zy_pass_on", A),
    ("zy_direct", B),
    ("zy_pass_on", B),
    ("yz_far", C),
    ("zy_across", A),
    ("yz_direct", C),
    ("zy_across", B),
    ("yz_pass_on", C),
    ("update", A),
    ("gather_y", A),
    ("gather_z", A, 0),
    ("gather_own", A, 0),
    ("update", B),
    ("gather_y", B),
    ("update", C),
    ("gather_z", C, 0),
    ("gather_y", C),
    ("gather_z", B, 0),
    ("gather_own", B, 0),
    ("gather_own", C, 0),
    ("came", A, 0, "up"),
    ("came", A, 0, "down"),
    ("came_across", A, "own"),
    ("gather_z", A, 1),
    ("came", C, 0, "up"),
    ("came", A, 0, "on"),
    ("came", C, 0, "down"),
    ("came_across", B, "own"),
    ("gather_z", B, 1),
    ("came", C, 0, "on"),
    ("came", B, 0, "up"),
    ("came", B, 0, "down"),
    ("came_across", C, "own"),
    ("came", A, 1, "up"),
    ("came", A, 1, "down"),
    ("came_across", C, "up"),
    ("came", B, 0, "on"),
    ("came", B, 1, "up"),
    ("came", A, 1, "on"),
    ("came_across", C, "down"),
    ("came", B, 1, "down"),
    ("came", B, 1, "on"),
    ("came_across", C, "on"),
)


def part_shape(p):
    array, _, rows = PARTS[p]
    return (rows, BLOCKS[array][1])


def outer_kernel(*refs):
    f32, bf16 = jnp.float32, jnp.bfloat16
    delta, master, moment = refs[0:9:3], refs[1:9:3], refs[2:9:3]
    params, new_master, new_moment = refs[9:18:3], refs[10:18:3], refs[11:18:3]
    n = len(PARTS)
    own, give, peer = refs[18:21], refs[21:24], refs[24:27]
    far, direct, summed, across = (refs[27 + n * i : 27 + n * (i + 1)] for i in range(4))
    rest = refs[27 + 4 * n :]
    held_master, held_moment = rest[0:3], rest[3:6]
    size, load_sem, send_sem, recv_sem = rest[6:]

    yh, z, c = (lax.axis_index(a) for a in REP)
    zs = [lax.rem(z + k, 4) for k in range(4)]
    ys = [yh, 1 - yh]
    core_to, y_to = {"c": 1 - c}, {"yh": 1 - yh}
    z_to = {1: {"z": zs[1]}, 3: {"z": zs[3]}}
    up, down = (1, 3), (3, 1)

    barrier = pltpu.get_barrier_semaphore()
    for to in (y_to, z_to[1], z_to[3], core_to):
        pl.semaphore_signal(barrier, inc=1, device_id=to, device_id_type=MESH)

    def wait_bytes(sem, total):
        piece = size.at[pl.ds(0, total // 256)]
        pltpu.make_async_remote_copy(
            src_ref=piece,
            dst_ref=piece,
            send_sem=sem,
            recv_sem=sem,
            device_id=core_to,
            device_id_type=MESH,
        ).wait_recv()

    groups, sent, load_bytes = {}, [0] * SENDS, [0] * LOADS

    def send(src, dst, to, group, which):
        index, total = groups.get(group, (len(groups), 0))
        count = 2 * math.prod(src.shape)
        groups[group] = (index, total + count)
        sent[which] += count
        pltpu.make_async_remote_copy(
            src_ref=src,
            dst_ref=dst,
            send_sem=send_sem.at[which],
            recv_sem=recv_sem.at[index],
            device_id=to,
            device_id_type=MESH,
        ).start()

    def arrive(*group):
        index, total = groups[group]
        wait_bytes(recv_sem.at[index], total)

    def load(src, dst, which, width):
        load_bytes[which] += width * math.prod(src.shape)
        pltpu.make_async_copy(src, dst, load_sem.at[which]).start()

    def block(ref, p, layer, y, zz, core):
        array, first, rows = PARTS[p]
        if array < 2:
            return ref[array].at[layer, y, zz, core, pl.ds(first, rows)]
        column = pl.multiple_of(((y * 4 + zz) * 2 + core) * 128, 128)
        return ref[2].at[layer, pl.ds(first, rows), pl.ds(column, 128)]

    both = slice(None)

    def at(ref, p, l, k, y):
        array, first, rows = PARTS[p]
        return ref[array].at[l, k, y, pl.ds(first, rows)]

    for k in (2, 1, 3, 0):
        which = (2, 1, 0, 1)[k]
        for mine, ref, core in ((False, give, 1 - c), (True, own, c)):
            for a in range(3):
                if a < 2:
                    load(delta[a].at[:, :, zs[k], core], ref[a].at[:, k], which, 2)
                else:
                    for y in (0, 1):
                        column = pl.multiple_of(((y * 4 + zs[k]) * 2 + core) * 128, 128)
                        load(delta[a].at[:, :, pl.ds(column, 128)], ref[a].at[:, k, y], which, 2)
    for a in range(3):
        load(master[a], held_master[a], 3, 4)
        load(moment[a], held_moment[a], 3, 4)

    pl.semaphore_wait(barrier, 4)

    mate = ys[1]
    order = (
        (A, (2,), "both"),
        (C, (2,), "mate"),
        (A, (1, 3), "both"),
        (C, (1, 3), "mate"),
        (B, (2,), "both"),
        (C, (0,), "mate"),
        (B, (1, 3), "both"),
        (A, (0,), "both"),
        (C, (2, 1, 3), "mine"),
        (B, (0,), "both"),
        (C, (0,), "mine"),
    )
    place = {"both": both, "mate": mate, "mine": yh}
    for step, (chunk, ks, y) in enumerate(order):
        if step in (0, 2, 5):
            which = (0, 2, 5).index(step)
            wait_bytes(load_sem.at[which], load_bytes[which])
        for p in chunk:
            for k in ks:
                send(
                    at(give, p, both, k, place[y]),
                    at(peer, p, both, k, place[y]),
                    core_to,
                    ("core", step),
                    0,
                )

    def pair(step):
        chunk, ks, y = order[step]
        arrive("core", step)
        for p in chunk:
            for k in ks:
                total = at(own, p, both, k, place[y])
                total[...] = total[...] + at(peer, p, both, k, place[y])[...]

    def total_of(*pieces):
        return sum(piece.astype(f32) for piece in pieces)

    layers = range(LAYERS)

    def zy_far(chunk):
        for l in layers:
            for p in chunk:
                send(at(own, p, l, 2, both), far[p].at[l], z_to[up[l]], ("far", chunk), 1)

    def zy_direct(chunk):
        for l in layers:
            for p in chunk:
                k = down[l]
                send(at(own, p, l, k, both), direct[p].at[l], z_to[k], ("direct", chunk), 1)

    def zy_pass_on(chunk):
        arrive("far", chunk)
        for l in layers:
            for p in chunk:
                k = up[l]
                total = at(own, p, l, k, both)
                total[...] = total_of(total[...], far[p][l]).astype(bf16)
                send(total, summed[p].at[l], z_to[k], ("summed", chunk), 1)

    def zy_across(chunk):
        arrive("direct", chunk)
        arrive("summed", chunk)
        for p in chunk:
            for l in layers:
                total = at(own, p, l, 0, mate)
                total[...] = total_of(total[...], direct[p][l, mate], summed[p][l, mate]).astype(
                    bf16
                )
            send(at(own, p, both, 0, mate), across[p].at[:, 0], y_to, ("y", chunk), 1)

    def yz_across(chunk, k):
        for p in chunk:
            send(at(own, p, both, k, mate), across[p].at[:, k], y_to, ("y", chunk, k), 1)

    def yz_far(chunk):
        arrive("y", chunk, 2)
        for l in layers:
            for p in chunk:
                total = at(own, p, l, 2, yh)
                total[...] = total[...] + across[p][l, 2]
                send(total, far[p].at[l, 0], z_to[up[l]], ("far", chunk), 1)

    def yz_direct(chunk):
        arrive("y", chunk, 1)
        arrive("y", chunk, 3)
        for l in layers:
            for p in chunk:
                k = down[l]
                total = at(own, p, l, k, yh)
                total[...] = total[...] + across[p][l, k]
                send(total, direct[p].at[l, 0], z_to[k], ("direct", chunk), 1)

    def yz_pass_on(chunk):
        arrive("far", chunk)
        for l in layers:
            for p in chunk:
                k = up[l]
                total = at(own, p, l, k, yh)
                total[...] = total_of(total[...], across[p][l, k], far[p][l, 0]).astype(bf16)
                send(total, summed[p].at[l, 0], z_to[k], ("summed", chunk), 1)

    state_here = []

    def update(chunk):
        if not state_here:
            wait_bytes(load_sem.at[3], load_bytes[3])
            state_here.append(True)
        if chunk in Z_FIRST:
            arrive("y", chunk)
        else:
            arrive("y", chunk, 0)
            arrive("direct", chunk)
            arrive("summed", chunk)
        for p in chunk:
            a, first, rows = PARTS[p]
            for l in layers:
                here = (l, pl.ds(first, rows))
                j = yh if chunk in Z_FIRST else 0
                total = total_of(
                    at(own, p, l, 0, yh)[...], direct[p][l, j], summed[p][l, j], across[p][l, 0]
                )
                average = total * (1.0 / REPLICAS)
                momentum = OUTER_MOMENTUM * held_moment[a][here] + average
                updated = held_master[a][here] - OUTER_RATE * (
                    average + OUTER_MOMENTUM * momentum
                )
                new_moment[a][here] = momentum
                new_master[a][here] = updated
                block(params, p, l, yh, z, c)[...] = updated.astype(bf16)

    def share(p, l, y, zz, to, group, which=2):
        piece = block(params, p, l, y, zz, c)
        send(piece, piece, to, group, which)

    def core_share(p, l, j, k):
        share(p, l, ys[j], zs[k], core_to, ("core",), 3)

    def gather_z(chunk, j):
        for name, way in (("up", up), ("down", down)):
            for l in layers:
                for p in chunk:
                    share(p, l, ys[j], z, z_to[way[l]], (name, chunk, j))

    def gather_own(chunk, j):
        for p in chunk:
            core_share(p, both, j, 0)

    def gather_y(chunk):
        for p in chunk:
            share(p, both, yh, z, y_to, ("across", chunk, "own"))

    def came(chunk, j, name):
        arrive(name, chunk, j)
        for l in layers:
            k = {"up": down[l], "down": up[l], "on": 2}[name]
            for p in chunk:
                if name == "up":
                    share(p, l, ys[j], zs[k], z_to[up[l]], ("on", chunk, j))
        for l in layers:
            k = {"up": down[l], "down": up[l], "on": 2}[name]
            for p in chunk:
                if chunk in Y_FIRST:
                    share(p, l, yh, zs[k], y_to, ("across", chunk, name))
                core_share(p, l, j, k)

    def came_across(chunk, name):
        arrive("across", chunk, name)
        for l in layers:
            k = {"own": 0, "up": down[l], "down": up[l], "on": 2}[name]
            for p in chunk:
                core_share(p, l, 1, k)

    stages = dict(
        pair=pair,
        zy_far=zy_far,
        zy_direct=zy_direct,
        zy_pass_on=zy_pass_on,
        zy_across=zy_across,
        yz_across=yz_across,
        yz_far=yz_far,
        yz_direct=yz_direct,
        yz_pass_on=yz_pass_on,
        update=update,
        gather_y=gather_y,
        gather_z=gather_z,
        gather_own=gather_own,
        came=came,
        came_across=came_across,
    )
    for name, *rest in SCHEDULE:
        stages[name](*rest)
    arrive("core")
    for which in range(SENDS):
        wait_bytes(send_sem.at[which], sent[which])


def write_kernel(*refs):
    sources, results, sem = refs[:9], refs[9:18], refs[18]
    copies = []
    for source, result in zip(sources, results):
        for layer in range(LAYERS):
            copies.append(
                pltpu.make_async_copy(source.at[layer], result.at[layer], sem.at[len(copies)])
            )
    for copy in copies:
        copy.start()
    for copy in copies:
        copy.wait()


def outer_step(
    delta_query,
    master_query,
    moment_query,
    delta_latent,
    master_latent,
    moment_latent,
    delta_output,
    master_output,
    moment_output,
):
    f32, bf16 = jnp.float32, jnp.bfloat16
    shapes = []
    for a, block in enumerate(BLOCKS):
        whole = (LAYERS, 2, 4, 2, *block) if a < 2 else (LAYERS, block[0], 16 * block[1])
        shapes += [(whole, bf16), ((LAYERS, *block), f32), ((LAYERS, *block), f32)]
    z_first = {p for chunk in Z_FIRST for p in chunk}
    scratch = []
    scratch += [pltpu.VMEM((LAYERS, 4, 2, *block), bf16) for _ in range(3) for block in BLOCKS]
    for kind in range(4):
        for p in range(len(PARTS)):
            if kind < 3:
                lead = (LAYERS, 2 if p in z_first else 1)
            else:
                lead = (LAYERS, 1 if p in z_first else 4)
            scratch.append(pltpu.VMEM((*lead, *part_shape(p)), bf16))
    scratch += [pltpu.VMEM((LAYERS, *block), f32) for _ in range(2) for block in BLOCKS]
    operands = (
        delta_query.reshape(shapes[0][0]),
        master_query,
        moment_query,
        delta_latent.reshape(shapes[3][0]),
        master_latent,
        moment_latent,
        delta_output.reshape(shapes[6][0]),
        master_output,
        moment_output,
    )
    operands = [pltpu.with_memory_space_constraint(x, pltpu.HBM) for x in operands]
    results = pl.pallas_call(
        outer_kernel,
        out_shape=tuple(pltpu.VMEM(*shape) for shape in shapes),
        in_specs=[pl.BlockSpec(memory_space=pltpu.HBM)] * 9,
        out_specs=tuple(pl.BlockSpec(memory_space=pltpu.VMEM) for _ in range(9)),
        scratch_shapes=scratch
        + [
            pltpu.VMEM((SIZE_ROWS, 128), bf16),
            pltpu.SemaphoreType.DMA((LOADS,)),
            pltpu.SemaphoreType.DMA((SENDS,)),
            pltpu.SemaphoreType.DMA((GROUPS,)),
        ],
        compiler_params=pltpu.CompilerParams(
            collective_id=0, has_side_effects=True, vmem_limit_bytes=40 * 1024 * 1024
        ),
    )(*operands)
    results = [pltpu.with_memory_space_constraint(x, pltpu.VMEM) for x in results]
    results = pl.pallas_call(
        write_kernel,
        out_shape=tuple(pltpu.HBM(*shape) for shape in shapes),
        in_specs=[pl.BlockSpec(memory_space=pltpu.VMEM)] * 9,
        out_specs=tuple(pl.BlockSpec(memory_space=pltpu.HBM) for _ in range(9)),
        scratch_shapes=[pltpu.SemaphoreType.DMA((9 * LAYERS,))],
        compiler_params=pltpu.CompilerParams(vmem_limit_bytes=4 * 1024 * 1024),
    )(*results)
    query, latent = results[0], results[3]
    return (
        query.reshape(LAYERS, 2048, 384),
        *results[1:3],
        latent.reshape(LAYERS, 512, 512),
        *results[4:],
    )


def solution(mesh):
    torus = Mesh(mesh.devices.reshape(2, 4, 2, 2, 4), (*REP, *TP))
    return jax.shard_map(
        outer_step,
        mesh=torus,
        in_specs=(
            P(REP, None, None, TP),
            P(None, REP, TP),
            P(None, REP, TP),
            P(REP, None, None, TP),
            P(None, REP, TP),
            P(None, REP, TP),
            P(REP, None, TP, None),
            P(None, TP, REP),
            P(None, TP, REP),
        ),
        out_specs=(
            P(None, None, TP),
            P(None, REP, TP),
            P(None, REP, TP),
            P(None, None, TP),
            P(None, REP, TP),
            P(None, REP, TP),
            P(None, TP, None),
            P(None, TP, REP),
            P(None, TP, REP),
        ),
        check_vma=False,
    )
```

```python
import math

import jax
import jax.numpy as jnp
from jax import lax
from jax.experimental import pallas as pl
from jax.experimental.pallas import tpu as pltpu
from jax.sharding import Mesh
from jax.sharding import PartitionSpec as P

REP = ("yh", "z", "c")
TP = ("yl", "x")
MESH = pl.DeviceIdType.MESH

OUTER_RATE = 0.7
OUTER_MOMENTUM = 0.9
REPLICAS = 16
LAYERS = 2

BLOCKS = ((128, 384), (32, 512), (256, 128))
PARTS = (
    (0, 0, 48),
    (0, 48, 48),
    (0, 96, 32),
    (1, 0, 16),
    (1, 16, 16),
    (2, 0, 256),
)
A, B, C, D = (0,), (1,), (2, 3), (4, 5)
Z_FIRST, Y_FIRST = (A, B, C,), (D,)
ORDER = (
    (A, (2,), "both"),
    (D, (2,), "mate"),
    (A, (1, 3), "both"),
    (B, (2,), "both"),
    (C, (2,), "both"),
    (D, (1, 3), "mate"),
    (B, (1, 3), "both"),
    (C, (1, 3), "both"),
    (D, (0,), "mate"),
    (D, (2, 1, 3), "mine"),
    (A, (0,), "both"),
    (B, (0,), "both"),
    (C, (0,), "both"),
    (D, (0,), "mine"),
)
GROUPS = 62
SENDS = 4
LOADS = 4
SIZE_ROWS = 3 * 4096


SCHEDULE = (
    ("pair", 0),
    ("zy_far", A),
    ("pair", 1),
    ("yz_across", D, 2),
    ("pair", 4),
    ("pair", 3),
    ("zy_far", B),
    ("pair", 5),
    ("yz_across", D, 3),
    ("pair", 6),
    ("zy_far", C),
    ("pair", 11),
    ("pair", 12),
    ("pair", 7),
    ("pair", 8),
    ("pair", 2),
    ("zy_direct", A),
    ("yz_across", D, 1),
    ("zy_pass_on", B),
    ("zy_direct", B),
    ("zy_pass_on", C),
    ("yz_across", D, 0),
    ("zy_direct", C),
    ("pair", 10),
    ("pair", 9),
    ("yz_far", D),
    ("zy_pass_on", A),
    ("yz_direct", D),
    ("zy_across", B),
    ("zy_across", C),
    ("yz_pass_on", D),
    ("pair", 13),
    ("update", B),
    ("gather_y", B),
    ("gather_z", B, 0),
    ("zy_across", A),
    ("update", C),
    ("gather_y", C),
    ("gather_z", C, 0),
    ("update", D),
    ("gather_own", D, 0),
    ("gather_z", D, 0),
    ("gather_y", D),
    ("came", B, 0, "up"),
    ("update", A),
    ("gather_z", A, 0),
    ("came_across", C, "own"),
    ("gather_y", A),
    ("came", C, 0, "up"),
    ("came", D, 0, "up"),
    ("came_across", B, "own"),
    ("gather_z", B, 1),
    ("came", B, 0, "down"),
    ("came", D, 0, "down"),
    ("came_across", A, "own"),
    ("gather_z", A, 1),
    ("came", D, 0, "on"),
    ("gather_z", C, 1),
    ("came", A, 0, "up"),
    ("gather_own", C, 0),
    ("came", A, 1, "up"),
    ("came", B, 1, "up"),
    ("came", A, 0, "down"),
    ("came_across", D, "up"),
    ("came", C, 1, "up"),
    ("came_across", D, "own"),
    ("came", B, 1, "down"),
    ("came", C, 1, "down"),
    ("came", A, 1, "down"),
    ("came", B, 0, "on"),
    ("came_across", D, "down"),
    ("gather_own", B, 0),
    ("gather_own", A, 0),
    ("came", C, 0, "on"),
    ("came", B, 1, "on"),
    ("came", A, 0, "on"),
    ("came", A, 1, "on"),
    ("came", C, 0, "down"),
    ("came_across", D, "on"),
    ("came", C, 1, "on"),
)


def part_shape(p):
    array, _, rows = PARTS[p]
    return (rows, BLOCKS[array][1])


def outer_kernel(*refs):
    f32, bf16 = jnp.float32, jnp.bfloat16
    delta, master, moment = refs[0:9:3], refs[1:9:3], refs[2:9:3]
    params, new_master, new_moment = refs[9:18:3], refs[10:18:3], refs[11:18:3]
    n = len(PARTS)
    own, give, peer = refs[18:21], refs[21:24], refs[24:27]
    far, direct, summed, across = (refs[27 + n * i : 27 + n * (i + 1)] for i in range(4))
    rest = refs[27 + 4 * n :]
    held_master, held_moment = rest[0:3], rest[3:6]
    size, load_sem, send_sem, recv_sem = rest[6:]

    yh, z, c = (lax.axis_index(a) for a in REP)
    zs = [lax.rem(z + k, 4) for k in range(4)]
    ys = [yh, 1 - yh]
    core_to, y_to = {"c": 1 - c}, {"yh": 1 - yh}
    z_to = {1: {"z": zs[1]}, 3: {"z": zs[3]}}
    up, down = (1, 3), (3, 1)

    barrier = pltpu.get_barrier_semaphore()
    for to in (y_to, z_to[1], z_to[3], core_to):
        pl.semaphore_signal(barrier, inc=1, device_id=to, device_id_type=MESH)

    def wait_bytes(sem, total):
        piece = size.at[pl.ds(0, total // 256)]
        pltpu.make_async_remote_copy(
            src_ref=piece,
            dst_ref=piece,
            send_sem=sem,
            recv_sem=sem,
            device_id=core_to,
            device_id_type=MESH,
        ).wait_recv()

    groups, sent, load_bytes = {}, [0] * SENDS, [0] * LOADS

    def send(src, dst, to, group, which):
        index, total = groups.get(group, (len(groups), 0))
        count = 2 * math.prod(src.shape)
        groups[group] = (index, total + count)
        sent[which] += count
        pltpu.make_async_remote_copy(
            src_ref=src,
            dst_ref=dst,
            send_sem=send_sem.at[which],
            recv_sem=recv_sem.at[index],
            device_id=to,
            device_id_type=MESH,
        ).start()

    def arrive(*group):
        index, total = groups[group]
        wait_bytes(recv_sem.at[index], total)

    def load(src, dst, which, width):
        load_bytes[which] += width * math.prod(src.shape)
        pltpu.make_async_copy(src, dst, load_sem.at[which]).start()

    def block(ref, p, layer, y, zz, core):
        array, first, rows = PARTS[p]
        if array < 2:
            return ref[array].at[layer, y, zz, core, pl.ds(first, rows)]
        column = pl.multiple_of(((y * 4 + zz) * 2 + core) * 128, 128)
        return ref[2].at[layer, pl.ds(first, rows), pl.ds(column, 128)]

    both = slice(None)

    def at(ref, p, l, k, y):
        array, first, rows = PARTS[p]
        return ref[array].at[l, k, y, pl.ds(first, rows)]

    for k in (2, 1, 3, 0):
        which = (2, 1, 0, 1)[k]
        for mine, ref, core in ((False, give, 1 - c), (True, own, c)):
            for a in range(3):
                if a < 2:
                    load(delta[a].at[:, :, zs[k], core], ref[a].at[:, k], which, 2)
                else:
                    for y in (0, 1):
                        column = pl.multiple_of(((y * 4 + zs[k]) * 2 + core) * 128, 128)
                        load(delta[a].at[:, :, pl.ds(column, 128)], ref[a].at[:, k, y], which, 2)
    for a in range(3):
        load(master[a], held_master[a], 3, 4)
        load(moment[a], held_moment[a], 3, 4)

    pl.semaphore_wait(barrier, 4)

    mate = ys[1]
    place = {"both": both, "mate": mate, "mine": yh}
    loaded = set()
    for step, (chunk, ks, y) in enumerate(ORDER):
        for k in ks:
            which = (2, 1, 0, 1)[k]
            if which not in loaded:
                loaded.add(which)
                wait_bytes(load_sem.at[which], load_bytes[which])
        for p in chunk:
            for k in ks:
                send(
                    at(give, p, both, k, place[y]),
                    at(peer, p, both, k, place[y]),
                    core_to,
                    ("core", step),
                    0,
                )

    def pair(step):
        chunk, ks, y = ORDER[step]
        arrive("core", step)
        for p in chunk:
            for k in ks:
                total = at(own, p, both, k, place[y])
                total[...] = total[...] + at(peer, p, both, k, place[y])[...]

    def total_of(*pieces):
        return sum(piece.astype(f32) for piece in pieces)

    layers = range(LAYERS)

    def zy_far(chunk):
        for l in layers:
            for p in chunk:
                send(at(own, p, l, 2, both), far[p].at[l], z_to[up[l]], ("far", chunk), 1)

    def zy_direct(chunk):
        for l in layers:
            for p in chunk:
                k = down[l]
                send(at(own, p, l, k, both), direct[p].at[l], z_to[k], ("direct", chunk), 1)

    def zy_pass_on(chunk):
        arrive("far", chunk)
        for l in layers:
            for p in chunk:
                k = up[l]
                total = at(own, p, l, k, both)
                total[...] = total_of(total[...], far[p][l]).astype(bf16)
                send(total, summed[p].at[l], z_to[k], ("summed", chunk), 1)

    def zy_across(chunk):
        arrive("direct", chunk)
        arrive("summed", chunk)
        for p in chunk:
            for l in layers:
                total = at(own, p, l, 0, mate)
                total[...] = total_of(total[...], direct[p][l, mate], summed[p][l, mate]).astype(
                    bf16
                )
            send(at(own, p, both, 0, mate), across[p].at[:, 0], y_to, ("y", chunk), 1)

    def yz_across(chunk, k):
        for p in chunk:
            send(at(own, p, both, k, mate), across[p].at[:, k], y_to, ("y", chunk, k), 1)

    def yz_far(chunk):
        arrive("y", chunk, 2)
        for l in layers:
            for p in chunk:
                total = at(own, p, l, 2, yh)
                total[...] = total[...] + across[p][l, 2]
                send(total, far[p].at[l, 0], z_to[up[l]], ("far", chunk), 1)

    def yz_direct(chunk):
        arrive("y", chunk, 1)
        arrive("y", chunk, 3)
        for l in layers:
            for p in chunk:
                k = down[l]
                total = at(own, p, l, k, yh)
                total[...] = total[...] + across[p][l, k]
                send(total, direct[p].at[l, 0], z_to[k], ("direct", chunk), 1)

    def yz_pass_on(chunk):
        arrive("far", chunk)
        for l in layers:
            for p in chunk:
                k = up[l]
                total = at(own, p, l, k, yh)
                total[...] = total_of(total[...], across[p][l, k], far[p][l, 0]).astype(bf16)
                send(total, summed[p].at[l, 0], z_to[k], ("summed", chunk), 1)

    state_here = []

    def update(chunk):
        if not state_here:
            wait_bytes(load_sem.at[3], load_bytes[3])
            state_here.append(True)
        if chunk in Z_FIRST:
            arrive("y", chunk)
        else:
            arrive("y", chunk, 0)
            arrive("direct", chunk)
            arrive("summed", chunk)
        for p in chunk:
            a, first, rows = PARTS[p]
            for l in layers:
                here = (l, pl.ds(first, rows))
                j = yh if chunk in Z_FIRST else 0
                total = total_of(
                    at(own, p, l, 0, yh)[...], direct[p][l, j], summed[p][l, j], across[p][l, 0]
                )
                average = total * (1.0 / REPLICAS)
                momentum = OUTER_MOMENTUM * held_moment[a][here] + average
                updated = held_master[a][here] - OUTER_RATE * (
                    average + OUTER_MOMENTUM * momentum
                )
                new_moment[a][here] = momentum
                new_master[a][here] = updated
                block(params, p, l, yh, z, c)[...] = updated.astype(bf16)

    def share(p, l, y, zz, to, group, which=2):
        piece = block(params, p, l, y, zz, c)
        send(piece, piece, to, group, which)

    def core_share(p, l, j, k):
        share(p, l, ys[j], zs[k], core_to, ("core",), 3)

    def gather_z(chunk, j):
        for name, way in (("up", up), ("down", down)):
            for l in layers:
                for p in chunk:
                    share(p, l, ys[j], z, z_to[way[l]], (name, chunk, j))

    def gather_own(chunk, j):
        for p in chunk:
            core_share(p, both, j, 0)

    def gather_y(chunk):
        for p in chunk:
            share(p, both, yh, z, y_to, ("across", chunk, "own"))

    def came(chunk, j, name):
        arrive(name, chunk, j)
        for l in layers:
            k = {"up": down[l], "down": up[l], "on": 2}[name]
            for p in chunk:
                if name == "up":
                    share(p, l, ys[j], zs[k], z_to[up[l]], ("on", chunk, j))
        for l in layers:
            k = {"up": down[l], "down": up[l], "on": 2}[name]
            for p in chunk:
                if chunk in Y_FIRST:
                    share(p, l, yh, zs[k], y_to, ("across", chunk, name))
                core_share(p, l, j, k)

    def came_across(chunk, name):
        arrive("across", chunk, name)
        for l in layers:
            k = {"own": 0, "up": down[l], "down": up[l], "on": 2}[name]
            for p in chunk:
                core_share(p, l, 1, k)

    stages = dict(
        pair=pair,
        zy_far=zy_far,
        zy_direct=zy_direct,
        zy_pass_on=zy_pass_on,
        zy_across=zy_across,
        yz_across=yz_across,
        yz_far=yz_far,
        yz_direct=yz_direct,
        yz_pass_on=yz_pass_on,
        update=update,
        gather_y=gather_y,
        gather_z=gather_z,
        gather_own=gather_own,
        came=came,
        came_across=came_across,
    )
    for name, *rest in SCHEDULE:
        stages[name](*rest)
    arrive("core")
    for which in range(SENDS):
        wait_bytes(send_sem.at[which], sent[which])


def write_kernel(*refs):
    sources, results, sem = refs[:9], refs[9:18], refs[18]
    copies = []
    for source, result in zip(sources, results):
        for layer in range(LAYERS):
            copies.append(
                pltpu.make_async_copy(source.at[layer], result.at[layer], sem.at[len(copies)])
            )
    for copy in copies:
        copy.start()
    for copy in copies:
        copy.wait()


def outer_step(
    delta_query,
    master_query,
    moment_query,
    delta_latent,
    master_latent,
    moment_latent,
    delta_output,
    master_output,
    moment_output,
):
    f32, bf16 = jnp.float32, jnp.bfloat16
    shapes = []
    for a, block in enumerate(BLOCKS):
        whole = (LAYERS, 2, 4, 2, *block) if a < 2 else (LAYERS, block[0], 16 * block[1])
        shapes += [(whole, bf16), ((LAYERS, *block), f32), ((LAYERS, *block), f32)]
    z_first = {p for chunk in Z_FIRST for p in chunk}
    scratch = []
    scratch += [pltpu.VMEM((LAYERS, 4, 2, *block), bf16) for _ in range(3) for block in BLOCKS]
    for kind in range(4):
        for p in range(len(PARTS)):
            if kind < 3:
                lead = (LAYERS, 2 if p in z_first else 1)
            else:
                lead = (LAYERS, 1 if p in z_first else 4)
            scratch.append(pltpu.VMEM((*lead, *part_shape(p)), bf16))
    scratch += [pltpu.VMEM((LAYERS, *block), f32) for _ in range(2) for block in BLOCKS]
    operands = (
        delta_query.reshape(shapes[0][0]),
        master_query,
        moment_query,
        delta_latent.reshape(shapes[3][0]),
        master_latent,
        moment_latent,
        delta_output.reshape(shapes[6][0]),
        master_output,
        moment_output,
    )
    operands = [pltpu.with_memory_space_constraint(x, pltpu.HBM) for x in operands]
    results = pl.pallas_call(
        outer_kernel,
        out_shape=tuple(pltpu.VMEM(*shape) for shape in shapes),
        in_specs=[pl.BlockSpec(memory_space=pltpu.HBM)] * 9,
        out_specs=tuple(pl.BlockSpec(memory_space=pltpu.VMEM) for _ in range(9)),
        scratch_shapes=scratch
        + [
            pltpu.VMEM((SIZE_ROWS, 128), bf16),
            pltpu.SemaphoreType.DMA((LOADS,)),
            pltpu.SemaphoreType.DMA((SENDS,)),
            pltpu.SemaphoreType.DMA((GROUPS,)),
        ],
        compiler_params=pltpu.CompilerParams(
            collective_id=0, has_side_effects=True, vmem_limit_bytes=40 * 1024 * 1024
        ),
    )(*operands)
    results = [pltpu.with_memory_space_constraint(x, pltpu.VMEM) for x in results]
    results = pl.pallas_call(
        write_kernel,
        out_shape=tuple(pltpu.HBM(*shape) for shape in shapes),
        in_specs=[pl.BlockSpec(memory_space=pltpu.VMEM)] * 9,
        out_specs=tuple(pl.BlockSpec(memory_space=pltpu.HBM) for _ in range(9)),
        scratch_shapes=[pltpu.SemaphoreType.DMA((9 * LAYERS,))],
        compiler_params=pltpu.CompilerParams(vmem_limit_bytes=4 * 1024 * 1024),
    )(*results)
    query, latent = results[0], results[3]
    return (
        query.reshape(LAYERS, 2048, 384),
        *results[1:3],
        latent.reshape(LAYERS, 512, 512),
        *results[4:],
    )


def solution(mesh):
    torus = Mesh(mesh.devices.reshape(2, 4, 2, 2, 4), (*REP, *TP))
    return jax.shard_map(
        outer_step,
        mesh=torus,
        in_specs=(
            P(REP, None, None, TP),
            P(None, REP, TP),
            P(None, REP, TP),
            P(REP, None, None, TP),
            P(None, REP, TP),
            P(None, REP, TP),
            P(REP, None, TP, None),
            P(None, TP, REP),
            P(None, TP, REP),
        ),
        out_specs=(
            P(None, None, TP),
            P(None, REP, TP),
            P(None, REP, TP),
            P(None, None, TP),
            P(None, REP, TP),
            P(None, REP, TP),
            P(None, TP, None),
            P(None, TP, REP),
            P(None, TP, REP),
        ),
        check_vma=False,
    )
```

```python
import math

import jax
import jax.numpy as jnp
from jax import lax
from jax.experimental import pallas as pl
from jax.experimental.pallas import tpu as pltpu
from jax.sharding import Mesh
from jax.sharding import PartitionSpec as P

REP = ("yh", "z", "c")
TP = ("yl", "x")
MESH = pl.DeviceIdType.MESH

OUTER_RATE = 0.7
OUTER_MOMENTUM = 0.9
REPLICAS = 16
LAYERS = 2

BLOCKS = ((128, 384), (32, 512), (256, 128))
PARTS = (
    (0, 0, 48),
    (0, 48, 48),
    (0, 96, 32),
    (2, 0, 48),
    (1, 0, 32),
    (2, 48, 208),
)
A, B, C, D = (0,), (1,), (2, 3), (4, 5)
Z_FIRST, Y_FIRST = (A, B, C,), (D,)
ORDER = (
    (A, (2,), "both"),
    (D, (2,), "mate"),
    (A, (1, 3), "both"),
    (B, (2,), "both"),
    (C, (2,), "both"),
    (D, (1, 3), "mate"),
    (B, (1, 3), "both"),
    (C, (1, 3), "both"),
    (D, (0,), "mate"),
    (D, (2, 1, 3), "mine"),
    (A, (0,), "both"),
    (B, (0,), "both"),
    (C, (0,), "both"),
    (D, (0,), "mine"),
)
GROUPS = 62
SENDS = 4
LOADS = 5
SIZE_ROWS = 3 * 4096


SCHEDULE = (
    ("pair", 0),
    ("zy_far", A),
    ("pair", 1),
    ("yz_across", D, 2),
    ("pair", 2),
    ("pair", 3),
    ("zy_far", B),
    ("pair", 6),
    ("zy_direct", B),
    ("pair", 5),
    ("yz_across", D, 3),
    ("pair", 4),
    ("pair", 11),
    ("zy_direct", A),
    ("zy_pass_on", A),
    ("pair", 10),
    ("yz_across", D, 1),
    ("pair", 7),
    ("zy_pass_on", B),
    ("pair", 9),
    ("zy_far", C),
    ("zy_direct", C),
    ("zy_across", A),
    ("yz_far", D),
    ("pair", 13),
    ("pair", 12),
    ("pair", 8),
    ("zy_across", B),
    ("zy_pass_on", C),
    ("yz_across", D, 0),
    ("yz_direct", D),
    ("update", A),
    ("yz_pass_on", D),
    ("gather_y", A),
    ("gather_z", A, 0),
    ("update", B),
    ("gather_z", B, 0),
    ("gather_y", B),
    ("zy_across", C),
    ("update", D),
    ("gather_y", D),
    ("gather_z", D, 0),
    ("came", B, 0, "up"),
    ("came_across", A, "own"),
    ("update", C),
    ("gather_y", C),
    ("came_across", B, "own"),
    ("gather_own", C, 0),
    ("gather_z", A, 1),
    ("came", D, 0, "up"),
    ("gather_z", B, 1),
    ("came_across", C, "own"),
    ("gather_z", C, 0),
    ("gather_own", D, 0),
    ("gather_own", A, 0),
    ("came", D, 0, "down"),
    ("gather_z", C, 1),
    ("came", B, 1, "up"),
    ("came", D, 0, "on"),
    ("came", A, 1, "up"),
    ("gather_own", B, 0),
    ("came", B, 0, "on"),
    ("came", B, 0, "down"),
    ("came", A, 0, "up"),
    ("came", B, 1, "down"),
    ("came", C, 0, "up"),
    ("came_across", D, "own"),
    ("came", C, 0, "down"),
    ("came", C, 1, "up"),
    ("came", A, 1, "on"),
    ("came", C, 1, "down"),
    ("came", A, 0, "on"),
    ("came", B, 1, "on"),
    ("came_across", D, "up"),
    ("came_across", D, "down"),
    ("came", A, 0, "down"),
    ("came", A, 1, "down"),
    ("came", C, 0, "on"),
    ("came_across", D, "on"),
    ("came", C, 1, "on"),
)


def part_shape(p):
    array, _, rows = PARTS[p]
    return (rows, BLOCKS[array][1])


def outer_kernel(*refs):
    f32, bf16 = jnp.float32, jnp.bfloat16
    delta, master, moment = refs[0:9:3], refs[1:9:3], refs[2:9:3]
    params, new_master, new_moment = refs[9:18:3], refs[10:18:3], refs[11:18:3]
    n = len(PARTS)
    own, give, peer = refs[18:21], refs[21:24], refs[24:27]
    far, direct, summed, across = (refs[27 + n * i : 27 + n * (i + 1)] for i in range(4))
    rest = refs[27 + 4 * n :]
    held_master, held_moment = rest[0:3], rest[3:6]
    size, load_sem, send_sem, recv_sem = rest[6:]

    yh, z, c = (lax.axis_index(a) for a in REP)
    zs = [lax.rem(z + k, 4) for k in range(4)]
    ys = [yh, 1 - yh]
    core_to, y_to = {"c": 1 - c}, {"yh": 1 - yh}
    z_to = {1: {"z": zs[1]}, 3: {"z": zs[3]}}
    up, down = (1, 3), (3, 1)

    barrier = pltpu.get_barrier_semaphore()
    for to in (y_to, z_to[1], z_to[3], core_to):
        pl.semaphore_signal(barrier, inc=1, device_id=to, device_id_type=MESH)

    def wait_bytes(sem, total):
        piece = size.at[pl.ds(0, total // 256)]
        pltpu.make_async_remote_copy(
            src_ref=piece,
            dst_ref=piece,
            send_sem=sem,
            recv_sem=sem,
            device_id=core_to,
            device_id_type=MESH,
        ).wait_recv()

    groups, sent, load_bytes = {}, [0] * SENDS, [0] * LOADS

    def send(src, dst, to, group, which):
        index, total = groups.get(group, (len(groups), 0))
        count = 2 * math.prod(src.shape)
        groups[group] = (index, total + count)
        sent[which] += count
        pltpu.make_async_remote_copy(
            src_ref=src,
            dst_ref=dst,
            send_sem=send_sem.at[which],
            recv_sem=recv_sem.at[index],
            device_id=to,
            device_id_type=MESH,
        ).start()

    def arrive(*group):
        index, total = groups[group]
        wait_bytes(recv_sem.at[index], total)

    def load(src, dst, which, width):
        load_bytes[which] += width * math.prod(src.shape)
        pltpu.make_async_copy(src, dst, load_sem.at[which]).start()

    def block(ref, p, layer, y, zz, core):
        array, first, rows = PARTS[p]
        if array < 2:
            return ref[array].at[layer, y, zz, core, pl.ds(first, rows)]
        column = pl.multiple_of(((y * 4 + zz) * 2 + core) * 128, 128)
        return ref[2].at[layer, pl.ds(first, rows), pl.ds(column, 128)]

    both = slice(None)

    def at(ref, p, l, k, y):
        array, first, rows = PARTS[p]
        return ref[array].at[l, k, y, pl.ds(first, rows)]

    first = PARTS[A[0]][2]
    top = pl.ds(0, first)
    for ref, core in ((give, 1 - c), (own, c)):
        load(delta[0].at[:, :, zs[2], core, top], ref[0].at[:, 2, :, top], 4, 2)
    for k in (2, 1, 3, 0):
        which = (2, 1, 0, 1)[k]
        for ref, core in ((give, 1 - c), (own, c)):
            for a in range(3):
                if a < 2:
                    below = pl.ds(first, BLOCKS[a][0] - first) if k == 2 and a == 0 else both
                    load(
                        delta[a].at[:, :, zs[k], core, below], ref[a].at[:, k, :, below], which, 2
                    )
                else:
                    for y in (0, 1):
                        column = pl.multiple_of(((y * 4 + zs[k]) * 2 + core) * 128, 128)
                        load(delta[a].at[:, :, pl.ds(column, 128)], ref[a].at[:, k, y], which, 2)
    for a in range(3):
        load(master[a], held_master[a], 3, 4)
        load(moment[a], held_moment[a], 3, 4)

    pl.semaphore_wait(barrier, 4)

    mate = ys[1]
    place = {"both": both, "mate": mate, "mine": yh}
    loaded = set()
    for step, (chunk, ks, y) in enumerate(ORDER):
        for k in ks:
            which = (2, 1, 0, 1)[k] if step else 4
            if which not in loaded:
                loaded.add(which)
                wait_bytes(load_sem.at[which], load_bytes[which])
        for p in chunk:
            for k in ks:
                send(
                    at(give, p, both, k, place[y]),
                    at(peer, p, both, k, place[y]),
                    core_to,
                    ("core", step),
                    0,
                )

    def pair(step):
        chunk, ks, y = ORDER[step]
        arrive("core", step)
        for p in chunk:
            for k in ks:
                total = at(own, p, both, k, place[y])
                total[...] = total[...] + at(peer, p, both, k, place[y])[...]

    def total_of(*pieces):
        return sum(piece.astype(f32) for piece in pieces)

    layers = range(LAYERS)

    def zy_far(chunk):
        for l in layers:
            for p in chunk:
                send(at(own, p, l, 2, both), far[p].at[l], z_to[up[l]], ("far", chunk), 1)

    def zy_direct(chunk):
        for l in layers:
            for p in chunk:
                k = down[l]
                send(at(own, p, l, k, both), direct[p].at[l], z_to[k], ("direct", chunk), 1)

    def zy_pass_on(chunk):
        arrive("far", chunk)
        for l in layers:
            for p in chunk:
                k = up[l]
                total = at(own, p, l, k, both)
                total[...] = total_of(total[...], far[p][l]).astype(bf16)
                send(total, summed[p].at[l], z_to[k], ("summed", chunk), 1)

    def zy_across(chunk):
        arrive("direct", chunk)
        arrive("summed", chunk)
        for p in chunk:
            for l in layers:
                total = at(own, p, l, 0, mate)
                total[...] = total_of(total[...], direct[p][l, mate], summed[p][l, mate]).astype(
                    bf16
                )
            send(at(own, p, both, 0, mate), across[p].at[:, 0], y_to, ("y", chunk), 1)

    def yz_across(chunk, k):
        for p in chunk:
            send(at(own, p, both, k, mate), across[p].at[:, k], y_to, ("y", chunk, k), 1)

    def yz_far(chunk):
        arrive("y", chunk, 2)
        for l in layers:
            for p in chunk:
                total = at(own, p, l, 2, yh)
                total[...] = total[...] + across[p][l, 2]
                send(total, far[p].at[l, 0], z_to[up[l]], ("far", chunk), 1)

    def yz_direct(chunk):
        arrive("y", chunk, 1)
        arrive("y", chunk, 3)
        for l in layers:
            for p in chunk:
                k = down[l]
                total = at(own, p, l, k, yh)
                total[...] = total[...] + across[p][l, k]
                send(total, direct[p].at[l, 0], z_to[k], ("direct", chunk), 1)

    def yz_pass_on(chunk):
        arrive("far", chunk)
        for l in layers:
            for p in chunk:
                k = up[l]
                total = at(own, p, l, k, yh)
                total[...] = total_of(total[...], across[p][l, k], far[p][l, 0]).astype(bf16)
                send(total, summed[p].at[l, 0], z_to[k], ("summed", chunk), 1)

    state_here = []

    def update(chunk):
        if not state_here:
            wait_bytes(load_sem.at[3], load_bytes[3])
            state_here.append(True)
        if chunk in Z_FIRST:
            arrive("y", chunk)
        else:
            arrive("y", chunk, 0)
            arrive("direct", chunk)
            arrive("summed", chunk)
        for p in chunk:
            a, first, rows = PARTS[p]
            for l in layers:
                here = (l, pl.ds(first, rows))
                j = yh if chunk in Z_FIRST else 0
                total = total_of(
                    at(own, p, l, 0, yh)[...], direct[p][l, j], summed[p][l, j], across[p][l, 0]
                )
                average = total * (1.0 / REPLICAS)
                momentum = OUTER_MOMENTUM * held_moment[a][here] + average
                updated = held_master[a][here] - OUTER_RATE * (
                    average + OUTER_MOMENTUM * momentum
                )
                new_moment[a][here] = momentum
                new_master[a][here] = updated
                block(params, p, l, yh, z, c)[...] = updated.astype(bf16)

    def share(p, l, y, zz, to, group, which=2):
        piece = block(params, p, l, y, zz, c)
        send(piece, piece, to, group, which)

    def core_share(p, l, j, k):
        share(p, l, ys[j], zs[k], core_to, ("core",), 3)

    def gather_z(chunk, j):
        for name, way in (("up", up), ("down", down)):
            for l in layers:
                for p in chunk:
                    share(p, l, ys[j], z, z_to[way[l]], (name, chunk, j))

    def gather_own(chunk, j):
        for p in chunk:
            core_share(p, both, j, 0)

    def gather_y(chunk):
        for p in chunk:
            share(p, both, yh, z, y_to, ("across", chunk, "own"))

    def came(chunk, j, name):
        arrive(name, chunk, j)
        for l in layers:
            k = {"up": down[l], "down": up[l], "on": 2}[name]
            for p in chunk:
                if name == "up":
                    share(p, l, ys[j], zs[k], z_to[up[l]], ("on", chunk, j))
        for l in layers:
            k = {"up": down[l], "down": up[l], "on": 2}[name]
            for p in chunk:
                if chunk in Y_FIRST:
                    share(p, l, yh, zs[k], y_to, ("across", chunk, name))
                core_share(p, l, j, k)

    def came_across(chunk, name):
        arrive("across", chunk, name)
        for l in layers:
            k = {"own": 0, "up": down[l], "down": up[l], "on": 2}[name]
            for p in chunk:
                core_share(p, l, 1, k)

    stages = dict(
        pair=pair,
        zy_far=zy_far,
        zy_direct=zy_direct,
        zy_pass_on=zy_pass_on,
        zy_across=zy_across,
        yz_across=yz_across,
        yz_far=yz_far,
        yz_direct=yz_direct,
        yz_pass_on=yz_pass_on,
        update=update,
        gather_y=gather_y,
        gather_z=gather_z,
        gather_own=gather_own,
        came=came,
        came_across=came_across,
    )
    for name, *rest in SCHEDULE:
        stages[name](*rest)
    arrive("core")
    for which in range(SENDS):
        wait_bytes(send_sem.at[which], sent[which])


def write_kernel(*refs):
    sources, results, sem = refs[:9], refs[9:18], refs[18]
    copies = []
    for source, result in zip(sources, results):
        for layer in range(LAYERS):
            copies.append(
                pltpu.make_async_copy(source.at[layer], result.at[layer], sem.at[len(copies)])
            )
    for copy in copies:
        copy.start()
    for copy in copies:
        copy.wait()


def outer_step(
    delta_query,
    master_query,
    moment_query,
    delta_latent,
    master_latent,
    moment_latent,
    delta_output,
    master_output,
    moment_output,
):
    f32, bf16 = jnp.float32, jnp.bfloat16
    shapes = []
    for a, block in enumerate(BLOCKS):
        whole = (LAYERS, 2, 4, 2, *block) if a < 2 else (LAYERS, block[0], 16 * block[1])
        shapes += [(whole, bf16), ((LAYERS, *block), f32), ((LAYERS, *block), f32)]
    z_first = {p for chunk in Z_FIRST for p in chunk}
    scratch = []
    scratch += [pltpu.VMEM((LAYERS, 4, 2, *block), bf16) for _ in range(3) for block in BLOCKS]
    for kind in range(4):
        for p in range(len(PARTS)):
            if kind < 3:
                lead = (LAYERS, 2 if p in z_first else 1)
            else:
                lead = (LAYERS, 1 if p in z_first else 4)
            scratch.append(pltpu.VMEM((*lead, *part_shape(p)), bf16))
    scratch += [pltpu.VMEM((LAYERS, *block), f32) for _ in range(2) for block in BLOCKS]
    operands = (
        delta_query.reshape(shapes[0][0]),
        master_query,
        moment_query,
        delta_latent.reshape(shapes[3][0]),
        master_latent,
        moment_latent,
        delta_output.reshape(shapes[6][0]),
        master_output,
        moment_output,
    )
    operands = [pltpu.with_memory_space_constraint(x, pltpu.HBM) for x in operands]
    results = pl.pallas_call(
        outer_kernel,
        out_shape=tuple(pltpu.VMEM(*shape) for shape in shapes),
        in_specs=[pl.BlockSpec(memory_space=pltpu.HBM)] * 9,
        out_specs=tuple(pl.BlockSpec(memory_space=pltpu.VMEM) for _ in range(9)),
        scratch_shapes=scratch
        + [
            pltpu.VMEM((SIZE_ROWS, 128), bf16),
            pltpu.SemaphoreType.DMA((LOADS,)),
            pltpu.SemaphoreType.DMA((SENDS,)),
            pltpu.SemaphoreType.DMA((GROUPS,)),
        ],
        compiler_params=pltpu.CompilerParams(
            collective_id=0, has_side_effects=True, vmem_limit_bytes=40 * 1024 * 1024
        ),
    )(*operands)
    results = [pltpu.with_memory_space_constraint(x, pltpu.VMEM) for x in results]
    results = pl.pallas_call(
        write_kernel,
        out_shape=tuple(pltpu.HBM(*shape) for shape in shapes),
        in_specs=[pl.BlockSpec(memory_space=pltpu.VMEM)] * 9,
        out_specs=tuple(pl.BlockSpec(memory_space=pltpu.HBM) for _ in range(9)),
        scratch_shapes=[pltpu.SemaphoreType.DMA((9 * LAYERS,))],
        compiler_params=pltpu.CompilerParams(vmem_limit_bytes=4 * 1024 * 1024),
    )(*results)
    query, latent = results[0], results[3]
    return (
        query.reshape(LAYERS, 2048, 384),
        *results[1:3],
        latent.reshape(LAYERS, 512, 512),
        *results[4:],
    )


def solution(mesh):
    torus = Mesh(mesh.devices.reshape(2, 4, 2, 2, 4), (*REP, *TP))
    return jax.shard_map(
        outer_step,
        mesh=torus,
        in_specs=(
            P(REP, None, None, TP),
            P(None, REP, TP),
            P(None, REP, TP),
            P(REP, None, None, TP),
            P(None, REP, TP),
            P(None, REP, TP),
            P(REP, None, TP, None),
            P(None, TP, REP),
            P(None, TP, REP),
        ),
        out_specs=(
            P(None, None, TP),
            P(None, REP, TP),
            P(None, REP, TP),
            P(None, None, TP),
            P(None, REP, TP),
            P(None, REP, TP),
            P(None, TP, None),
            P(None, TP, REP),
            P(None, TP, REP),
        ),
        check_vma=False,
    )
```

```python
import math

import jax
import jax.numpy as jnp
from jax import lax
from jax.experimental import pallas as pl
from jax.experimental.pallas import tpu as pltpu
from jax.sharding import Mesh
from jax.sharding import PartitionSpec as P

REP = ("yh", "z", "c")
TP = ("yl", "x")
MESH = pl.DeviceIdType.MESH

OUTER_RATE = 0.7
OUTER_MOMENTUM = 0.9
REPLICAS = 16
LAYERS = 2

BLOCKS = ((128, 384), (32, 512), (256, 128))
PARTS = (
    (0, 0, 48),
    (0, 48, 48),
    (0, 96, 32),
    (2, 0, 48),
    (1, 0, 32),
    (2, 48, 208),
)
A, B, C, D = (0,), (1,), (2, 3), (4, 5)
Z_FIRST, Y_FIRST = (A, B, C,), (D,)
ORDER = (
    (A, (2,), "both"),
    (D, (2,), "mate"),
    (A, (1, 3), "both"),
    (B, (2,), "both"),
    (C, (2,), "both"),
    (D, (1, 3), "mate"),
    (B, (1, 3), "both"),
    (C, (1, 3), "both"),
    (D, (0,), "mate"),
    (D, (2, 1, 3), "mine"),
    (A, (0,), "both"),
    (B, (0,), "both"),
    (C, (0,), "both"),
    (D, (0,), "mine"),
)
LAST = 9
GROUPS = 52
SENDS = 4
LOADS = 5
SIZE_ROWS = 3 * 4096


SCHEDULE = (
    ("pair", 0),
    ("zy_far", A),
    ("pair", 1),
    ("yz_across", D, 2),
    ("pair", 2),
    ("pair", 3),
    ("zy_far", B),
    ("pair", 6),
    ("zy_direct", B),
    ("pair", 5),
    ("yz_across", D, 3),
    ("pair", 4),
    ("pair", 11),
    ("zy_direct", A),
    ("zy_pass_on", A),
    ("pair", 10),
    ("yz_across", D, 1),
    ("pair", 7),
    ("zy_pass_on", B),
    ("pair", 9),
    ("zy_far", C),
    ("zy_direct", C),
    ("zy_across", A),
    ("yz_far", D),
    ("pair", 13),
    ("pair", 12),
    ("pair", 8),
    ("zy_across", B),
    ("zy_pass_on", C),
    ("yz_across", D, 0),
    ("yz_direct", D),
    ("update", A),
    ("yz_pass_on", D),
    ("gather_y", A),
    ("gather_z", A, 0),
    ("update", B),
    ("gather_z", B, 0),
    ("gather_y", B),
    ("zy_across", C),
    ("update", D),
    ("gather_y", D),
    ("gather_z", D, 0),
    ("came", B, 0, "up"),
    ("came_across", A, "own"),
    ("update", C),
    ("gather_y", C),
    ("came_across", B, "own"),
    ("gather_own", C, 0),
    ("gather_z", A, 1),
    ("came", D, 0, "up"),
    ("gather_z", B, 1),
    ("came_across", C, "own"),
    ("gather_z", C, 0),
    ("gather_own", D, 0),
    ("gather_own", A, 0),
    ("came", D, 0, "down"),
    ("gather_z", C, 1),
    ("came", B, 1, "up"),
    ("came", D, 0, "on"),
    ("came", A, 1, "up"),
    ("gather_own", B, 0),
    ("came", B, 0, "on"),
    ("came", B, 0, "down"),
    ("came", A, 0, "up"),
    ("came", B, 1, "down"),
    ("came", C, 0, "up"),
    ("came_across", D, "own"),
    ("came", C, 0, "down"),
    ("came", C, 1, "up"),
    ("came", A, 1, "on"),
    ("came", C, 1, "down"),
    ("came", A, 0, "on"),
    ("came", B, 1, "on"),
    ("came_across", D, "up"),
    ("came_across", D, "down"),
    ("came", A, 0, "down"),
    ("came", A, 1, "down"),
    ("came", C, 0, "on"),
    ("came_across", D, "on"),
    ("came", C, 1, "on"),
)


def part_shape(p):
    array, _, rows = PARTS[p]
    return (rows, BLOCKS[array][1])


def outer_kernel(*refs):
    f32, bf16 = jnp.float32, jnp.bfloat16
    delta, master, moment = refs[0:9:3], refs[1:9:3], refs[2:9:3]
    params, new_master, new_moment = refs[9:18:3], refs[10:18:3], refs[11:18:3]
    n = len(PARTS)
    own, give, peer = refs[18:21], refs[21:24], refs[24:27]
    far, direct, summed, across = (refs[27 + n * i : 27 + n * (i + 1)] for i in range(4))
    rest = refs[27 + 4 * n :]
    held_master, held_moment = rest[0:3], rest[3:6]
    size, load_sem, send_sem, recv_sem = rest[6:]

    yh, z, c = (lax.axis_index(a) for a in REP)
    zs = [lax.rem(z + k, 4) for k in range(4)]
    ys = [yh, 1 - yh]
    core_to, y_to = {"c": 1 - c}, {"yh": 1 - yh}
    z_to = {1: {"z": zs[1]}, 3: {"z": zs[3]}}
    up, down = (1, 3), (3, 1)

    barrier = pltpu.get_barrier_semaphore()
    for to in (y_to, z_to[1], z_to[3], core_to):
        pl.semaphore_signal(barrier, inc=1, device_id=to, device_id_type=MESH)

    def wait_bytes(sem, total):
        piece = size.at[pl.ds(0, total // 256)]
        pltpu.make_async_remote_copy(
            src_ref=piece,
            dst_ref=piece,
            send_sem=sem,
            recv_sem=sem,
            device_id=core_to,
            device_id_type=MESH,
        ).wait_recv()

    groups, sent, load_bytes = {}, [0] * SENDS, [0] * LOADS

    def send(src, dst, to, group, which):
        index, total = groups.get(group, (len(groups), 0))
        count = 2 * math.prod(src.shape)
        groups[group] = (index, total + count)
        sent[which] += count
        pltpu.make_async_remote_copy(
            src_ref=src,
            dst_ref=dst,
            send_sem=send_sem.at[which],
            recv_sem=recv_sem.at[index],
            device_id=to,
            device_id_type=MESH,
        ).start()

    def arrive(*group):
        index, total = groups[group]
        wait_bytes(recv_sem.at[index], total)

    def load(src, dst, which, width):
        load_bytes[which] += width * math.prod(src.shape)
        pltpu.make_async_copy(src, dst, load_sem.at[which]).start()

    def block(ref, p, layer, y, zz, core):
        array, first, rows = PARTS[p]
        if array < 2:
            return ref[array].at[layer, y, zz, core, pl.ds(first, rows)]
        column = pl.multiple_of(((y * 4 + zz) * 2 + core) * 128, 128)
        return ref[2].at[layer, pl.ds(first, rows), pl.ds(column, 128)]

    both = slice(None)

    def at(ref, p, l, k, y):
        array, first, rows = PARTS[p]
        return ref[array].at[l, k, y, pl.ds(first, rows)]

    first = PARTS[A[0]][2]
    top = pl.ds(0, first)
    for ref, core in ((give, 1 - c), (own, c)):
        load(delta[0].at[:, :, zs[2], core, top], ref[0].at[:, 2, :, top], 4, 2)
    for k in (2, 1, 3, 0):
        which = (2, 1, 0, 1)[k]
        for ref, core in ((give, 1 - c), (own, c)):
            for a in range(3):
                if a < 2:
                    below = pl.ds(first, BLOCKS[a][0] - first) if k == 2 and a == 0 else both
                    load(
                        delta[a].at[:, :, zs[k], core, below], ref[a].at[:, k, :, below], which, 2
                    )
                else:
                    for y in (0, 1):
                        column = pl.multiple_of(((y * 4 + zs[k]) * 2 + core) * 128, 128)
                        load(delta[a].at[:, :, pl.ds(column, 128)], ref[a].at[:, k, y], which, 2)
    for a in range(3):
        load(master[a], held_master[a], 3, 4)
        load(moment[a], held_moment[a], 3, 4)

    pl.semaphore_wait(barrier, 4)

    mate = ys[1]
    place = {"both": both, "mate": mate, "mine": yh}
    loaded = set()
    for step, (chunk, ks, y) in enumerate(ORDER):
        for k in ks:
            which = (2, 1, 0, 1)[k] if step else 4
            if which not in loaded:
                loaded.add(which)
                wait_bytes(load_sem.at[which], load_bytes[which])
        for p in chunk:
            for k in ks:
                send(
                    at(give, p, both, k, place[y]),
                    at(peer, p, both, k, place[y]),
                    core_to,
                    ("core", min(step, LAST)),
                    0,
                )

    paired = set()

    def pair(step):
        chunk, ks, y = ORDER[step]
        if min(step, LAST) not in paired:
            paired.add(min(step, LAST))
            arrive("core", min(step, LAST))
        for p in chunk:
            for k in ks:
                total = at(own, p, both, k, place[y])
                total[...] = total[...] + at(peer, p, both, k, place[y])[...]

    def total_of(*pieces):
        return sum(piece.astype(f32) for piece in pieces)

    layers = range(LAYERS)

    def zy_far(chunk):
        for l in layers:
            for p in chunk:
                send(at(own, p, l, 2, both), far[p].at[l], z_to[up[l]], ("far", chunk), 1)

    def zy_direct(chunk):
        for l in layers:
            for p in chunk:
                k = down[l]
                send(at(own, p, l, k, both), direct[p].at[l], z_to[k], ("final", chunk), 1)

    def zy_pass_on(chunk):
        arrive("far", chunk)
        for l in layers:
            for p in chunk:
                k = up[l]
                total = at(own, p, l, k, both)
                total[...] = total_of(total[...], far[p][l]).astype(bf16)
                send(total, summed[p].at[l], z_to[k], ("final", chunk), 1)

    def zy_across(chunk):
        arrive("final", chunk)
        for p in chunk:
            for l in layers:
                total = at(own, p, l, 0, mate)
                total[...] = total_of(total[...], direct[p][l, mate], summed[p][l, mate]).astype(
                    bf16
                )
            send(at(own, p, both, 0, mate), across[p].at[:, 0], y_to, ("y", chunk), 1)

    def yz_across(chunk, k):
        group = {0: ("final", chunk), 2: ("far y", chunk)}.get(k, ("side y", chunk))
        for p in chunk:
            send(at(own, p, both, k, mate), across[p].at[:, k], y_to, group, 1)

    def yz_far(chunk):
        arrive("far y", chunk)
        for l in layers:
            for p in chunk:
                total = at(own, p, l, 2, yh)
                total[...] = total[...] + across[p][l, 2]
                send(total, far[p].at[l, 0], z_to[up[l]], ("far", chunk), 1)

    def yz_direct(chunk):
        arrive("side y", chunk)
        for l in layers:
            for p in chunk:
                k = down[l]
                total = at(own, p, l, k, yh)
                total[...] = total[...] + across[p][l, k]
                send(total, direct[p].at[l, 0], z_to[k], ("final", chunk), 1)

    def yz_pass_on(chunk):
        arrive("far", chunk)
        for l in layers:
            for p in chunk:
                k = up[l]
                total = at(own, p, l, k, yh)
                total[...] = total_of(total[...], across[p][l, k], far[p][l, 0]).astype(bf16)
                send(total, summed[p].at[l, 0], z_to[k], ("final", chunk), 1)

    state_here = []

    def update(chunk):
        if not state_here:
            wait_bytes(load_sem.at[3], load_bytes[3])
            state_here.append(True)
        if chunk in Z_FIRST:
            arrive("y", chunk)
        else:
            arrive("final", chunk)
        for p in chunk:
            a, first, rows = PARTS[p]
            for l in layers:
                here = (l, pl.ds(first, rows))
                j = yh if chunk in Z_FIRST else 0
                total = total_of(
                    at(own, p, l, 0, yh)[...], direct[p][l, j], summed[p][l, j], across[p][l, 0]
                )
                average = total * (1.0 / REPLICAS)
                momentum = OUTER_MOMENTUM * held_moment[a][here] + average
                updated = held_master[a][here] - OUTER_RATE * (
                    average + OUTER_MOMENTUM * momentum
                )
                new_moment[a][here] = momentum
                new_master[a][here] = updated
                block(params, p, l, yh, z, c)[...] = updated.astype(bf16)

    def share(p, l, y, zz, to, group, which=2):
        piece = block(params, p, l, y, zz, c)
        send(piece, piece, to, group, which)

    def core_share(p, l, j, k):
        share(p, l, ys[j], zs[k], core_to, ("core",), 3)

    def gather_z(chunk, j):
        for name, way in (("up", up), ("down", down)):
            for l in layers:
                for p in chunk:
                    share(p, l, ys[j], z, z_to[way[l]], (name, chunk, j))

    def gather_own(chunk, j):
        for p in chunk:
            core_share(p, both, j, 0)

    def gather_y(chunk):
        for p in chunk:
            share(p, both, yh, z, y_to, ("across", chunk, "own"))

    def came(chunk, j, name):
        arrive(name, chunk, j)
        for l in layers:
            k = {"up": down[l], "down": up[l], "on": 2}[name]
            for p in chunk:
                if name == "up":
                    share(p, l, ys[j], zs[k], z_to[up[l]], ("on", chunk, j))
        for l in layers:
            k = {"up": down[l], "down": up[l], "on": 2}[name]
            for p in chunk:
                if chunk in Y_FIRST:
                    share(p, l, yh, zs[k], y_to, ("across", chunk, name))
                core_share(p, l, j, k)

    def came_across(chunk, name):
        arrive("across", chunk, name)
        for l in layers:
            k = {"own": 0, "up": down[l], "down": up[l], "on": 2}[name]
            for p in chunk:
                core_share(p, l, 1, k)

    stages = dict(
        pair=pair,
        zy_far=zy_far,
        zy_direct=zy_direct,
        zy_pass_on=zy_pass_on,
        zy_across=zy_across,
        yz_across=yz_across,
        yz_far=yz_far,
        yz_direct=yz_direct,
        yz_pass_on=yz_pass_on,
        update=update,
        gather_y=gather_y,
        gather_z=gather_z,
        gather_own=gather_own,
        came=came,
        came_across=came_across,
    )
    for name, *rest in SCHEDULE:
        stages[name](*rest)
    arrive("core")
    for which in range(SENDS):
        wait_bytes(send_sem.at[which], sent[which])


def write_kernel(*refs):
    sources, results, sem = refs[:9], refs[9:18], refs[18]
    copies = []
    for source, result in zip(sources, results):
        for layer in range(LAYERS):
            copies.append(
                pltpu.make_async_copy(source.at[layer], result.at[layer], sem.at[len(copies)])
            )
    for copy in copies:
        copy.start()
    for copy in copies:
        copy.wait()


def outer_step(
    delta_query,
    master_query,
    moment_query,
    delta_latent,
    master_latent,
    moment_latent,
    delta_output,
    master_output,
    moment_output,
):
    f32, bf16 = jnp.float32, jnp.bfloat16
    shapes = []
    for a, block in enumerate(BLOCKS):
        whole = (LAYERS, 2, 4, 2, *block) if a < 2 else (LAYERS, block[0], 16 * block[1])
        shapes += [(whole, bf16), ((LAYERS, *block), f32), ((LAYERS, *block), f32)]
    z_first = {p for chunk in Z_FIRST for p in chunk}
    scratch = []
    scratch += [pltpu.VMEM((LAYERS, 4, 2, *block), bf16) for _ in range(3) for block in BLOCKS]
    for kind in range(4):
        for p in range(len(PARTS)):
            if kind < 3:
                lead = (LAYERS, 2 if p in z_first else 1)
            else:
                lead = (LAYERS, 1 if p in z_first else 4)
            scratch.append(pltpu.VMEM((*lead, *part_shape(p)), bf16))
    scratch += [pltpu.VMEM((LAYERS, *block), f32) for _ in range(2) for block in BLOCKS]
    operands = (
        delta_query.reshape(shapes[0][0]),
        master_query,
        moment_query,
        delta_latent.reshape(shapes[3][0]),
        master_latent,
        moment_latent,
        delta_output.reshape(shapes[6][0]),
        master_output,
        moment_output,
    )
    operands = [pltpu.with_memory_space_constraint(x, pltpu.HBM) for x in operands]
    results = pl.pallas_call(
        outer_kernel,
        out_shape=tuple(pltpu.VMEM(*shape) for shape in shapes),
        in_specs=[pl.BlockSpec(memory_space=pltpu.HBM)] * 9,
        out_specs=tuple(pl.BlockSpec(memory_space=pltpu.VMEM) for _ in range(9)),
        scratch_shapes=scratch
        + [
            pltpu.VMEM((SIZE_ROWS, 128), bf16),
            pltpu.SemaphoreType.DMA((LOADS,)),
            pltpu.SemaphoreType.DMA((SENDS,)),
            pltpu.SemaphoreType.DMA((GROUPS,)),
        ],
        compiler_params=pltpu.CompilerParams(
            collective_id=0, has_side_effects=True, vmem_limit_bytes=40 * 1024 * 1024
        ),
    )(*operands)
    results = [pltpu.with_memory_space_constraint(x, pltpu.VMEM) for x in results]
    results = pl.pallas_call(
        write_kernel,
        out_shape=tuple(pltpu.HBM(*shape) for shape in shapes),
        in_specs=[pl.BlockSpec(memory_space=pltpu.VMEM)] * 9,
        out_specs=tuple(pl.BlockSpec(memory_space=pltpu.HBM) for _ in range(9)),
        scratch_shapes=[pltpu.SemaphoreType.DMA((9 * LAYERS,))],
        compiler_params=pltpu.CompilerParams(vmem_limit_bytes=4 * 1024 * 1024),
    )(*results)
    query, latent = results[0], results[3]
    return (
        query.reshape(LAYERS, 2048, 384),
        *results[1:3],
        latent.reshape(LAYERS, 512, 512),
        *results[4:],
    )


def solution(mesh):
    torus = Mesh(mesh.devices.reshape(2, 4, 2, 2, 4), (*REP, *TP))
    return jax.shard_map(
        outer_step,
        mesh=torus,
        in_specs=(
            P(REP, None, None, TP),
            P(None, REP, TP),
            P(None, REP, TP),
            P(REP, None, None, TP),
            P(None, REP, TP),
            P(None, REP, TP),
            P(REP, None, TP, None),
            P(None, TP, REP),
            P(None, TP, REP),
        ),
        out_specs=(
            P(None, None, TP),
            P(None, REP, TP),
            P(None, REP, TP),
            P(None, None, TP),
            P(None, REP, TP),
            P(None, REP, TP),
            P(None, TP, None),
            P(None, TP, REP),
            P(None, TP, REP),
        ),
        check_vma=False,
    )
```

```python
import math

import jax
import jax.numpy as jnp
from jax import lax
from jax.experimental import pallas as pl
from jax.experimental.pallas import tpu as pltpu
from jax.sharding import Mesh
from jax.sharding import PartitionSpec as P

REP = ("yh", "z", "c")
TP = ("yl", "x")
MESH = pl.DeviceIdType.MESH

OUTER_RATE = 0.7
OUTER_MOMENTUM = 0.9
REPLICAS = 16
LAYERS = 2

BLOCKS = ((128, 384), (32, 512), (256, 128))
PARTS = (
    (0, 0, 48),
    (0, 48, 48),
    (0, 96, 32),
    (2, 0, 48),
    (1, 0, 32),
    (2, 48, 208),
)
A, B, C, D = (0,), (1,), (2, 3), (4, 5)
Z_FIRST, Y_FIRST = (A, B, C,), (D,)
ORDER = (
    (A, (2,), "both"),
    (D, (2,), "mate"),
    (A, (1, 3), "both"),
    (B, (2,), "both"),
    (C, (2,), "both"),
    (D, (1, 3), "mate"),
    (B, (1, 3), "both"),
    (C, (1, 3), "both"),
    (D, (0,), "mate"),
    (D, (2, 1, 3), "mine"),
    (A, (0,), "both"),
    (B, (0,), "both"),
    (C, (0,), "both"),
    (D, (0,), "mine"),
)
LAST = 9
GROUPS = 52
SENDS = 4
LOADS = 5
SIZE_ROWS = 3 * 4096


SCHEDULE = (
    ("pair", 0),
    ("zy_far", A),
    ("pair", 1),
    ("yz_across", D, 2),
    ("pair", 2),
    ("pair", 3),
    ("zy_far", B),
    ("pair", 6),
    ("zy_direct", B),
    ("pair", 5),
    ("yz_across", D, 3),
    ("pair", 4),
    ("pair", 11),
    ("zy_direct", A),
    ("zy_pass_on", A),
    ("pair", 10),
    ("yz_across", D, 1),
    ("pair", 7),
    ("zy_pass_on", B),
    ("pair", 9),
    ("zy_far", C),
    ("zy_direct", C),
    ("zy_across", A),
    ("yz_far", D),
    ("pair", 13),
    ("pair", 12),
    ("pair", 8),
    ("zy_across", B),
    ("zy_pass_on", C),
    ("yz_across", D, 0),
    ("yz_direct", D),
    ("update", A),
    ("yz_pass_on", D),
    ("gather_y", A),
    ("gather_z", A, 0),
    ("update", B),
    ("gather_z", B, 0),
    ("gather_y", B),
    ("zy_across", C),
    ("update", D),
    ("gather_y", D),
    ("gather_z", D, 0),
    ("came", B, 0, "up"),
    ("came_across", A, "own"),
    ("update", C),
    ("gather_y", C),
    ("came_across", B, "own"),
    ("gather_own", C, 0),
    ("gather_z", A, 1),
    ("came", D, 0, "up"),
    ("gather_z", B, 1),
    ("came_across", C, "own"),
    ("gather_z", C, 0),
    ("gather_own", D, 0),
    ("gather_own", A, 0),
    ("came", D, 0, "down"),
    ("gather_z", C, 1),
    ("came", B, 1, "up"),
    ("came", D, 0, "on"),
    ("came", A, 1, "up"),
    ("gather_own", B, 0),
    ("came", B, 0, "on"),
    ("came", B, 0, "down"),
    ("came", A, 0, "up"),
    ("came", B, 1, "down"),
    ("came", C, 0, "up"),
    ("came_across", D, "own"),
    ("came", C, 0, "down"),
    ("came", C, 1, "up"),
    ("came", A, 1, "on"),
    ("came", C, 1, "down"),
    ("came", A, 0, "on"),
    ("came", B, 1, "on"),
    ("came_across", D, "up"),
    ("came_across", D, "down"),
    ("came", A, 0, "down"),
    ("came", A, 1, "down"),
    ("came", C, 0, "on"),
    ("came_across", D, "on"),
    ("came", C, 1, "on"),
)


def part_shape(p):
    array, _, rows = PARTS[p]
    return (rows, BLOCKS[array][1])


def outer_kernel(*refs):
    f32, bf16 = jnp.float32, jnp.bfloat16
    delta, master, moment = refs[0:9:3], refs[1:9:3], refs[2:9:3]
    params, new_master, new_moment = refs[9:18:3], refs[10:18:3], refs[11:18:3]
    n = len(PARTS)
    own, give, peer = refs[18:21], refs[21:24], refs[24:27]
    far, direct, summed, across = (refs[27 + n * i : 27 + n * (i + 1)] for i in range(4))
    rest = refs[27 + 4 * n :]
    held_master, held_moment = rest[0:3], rest[3:6]
    size, load_sem, send_sem, recv_sem = rest[6:]

    yh, z, c = (lax.axis_index(a) for a in REP)
    zs = [lax.rem(z + k, 4) for k in range(4)]
    ys = [yh, 1 - yh]
    core_to, y_to = {"c": 1 - c}, {"yh": 1 - yh}
    z_to = {1: {"z": zs[1]}, 3: {"z": zs[3]}}
    up, down = (1, 3), (3, 1)

    barrier = pltpu.get_barrier_semaphore()
    for to in (y_to, z_to[1], z_to[3], core_to):
        pl.semaphore_signal(barrier, inc=1, device_id=to, device_id_type=MESH)

    def wait_bytes(sem, total):
        piece = size.at[pl.ds(0, total // 256)]
        pltpu.make_async_remote_copy(
            src_ref=piece,
            dst_ref=piece,
            send_sem=sem,
            recv_sem=sem,
            device_id=core_to,
            device_id_type=MESH,
        ).wait_recv()

    groups, sent, load_bytes = {}, [0] * SENDS, [0] * LOADS

    def send(src, dst, to, group, which):
        index, total = groups.get(group, (len(groups), 0))
        count = 2 * math.prod(src.shape)
        groups[group] = (index, total + count)
        sent[which] += count
        pltpu.make_async_remote_copy(
            src_ref=src,
            dst_ref=dst,
            send_sem=send_sem.at[which],
            recv_sem=recv_sem.at[index],
            device_id=to,
            device_id_type=MESH,
        ).start()

    def arrive(*group):
        index, total = groups[group]
        wait_bytes(recv_sem.at[index], total)

    def load(src, dst, which, width):
        load_bytes[which] += width * math.prod(src.shape)
        pltpu.make_async_copy(src, dst, load_sem.at[which]).start()

    def block(ref, p, layer, y, zz, core):
        array, first, rows = PARTS[p]
        if array < 2:
            return ref[array].at[layer, y, zz, core, pl.ds(first, rows)]
        column = pl.multiple_of(((y * 4 + zz) * 2 + core) * 128, 128)
        return ref[2].at[layer, pl.ds(first, rows), pl.ds(column, 128)]

    both = slice(None)

    def at(ref, p, l, k, y):
        array, first, rows = PARTS[p]
        return ref[array].at[l, k, y, pl.ds(first, rows)]

    first = PARTS[A[0]][2]
    top = pl.ds(0, first)
    for ref, core in ((give, 1 - c), (own, c)):
        load(delta[0].at[:, :, zs[2], core, top], ref[0].at[:, 2, :, top], 4, 2)
    for k in (2, 1, 3, 0):
        which = (2, 1, 0, 1)[k]
        for ref, core in ((give, 1 - c), (own, c)):
            for a in range(3):
                if a < 2:
                    below = pl.ds(first, BLOCKS[a][0] - first) if k == 2 and a == 0 else both
                    load(
                        delta[a].at[:, :, zs[k], core, below], ref[a].at[:, k, :, below], which, 2
                    )
                else:
                    for y in (0, 1):
                        column = pl.multiple_of(((y * 4 + zs[k]) * 2 + core) * 128, 128)
                        load(delta[a].at[:, :, pl.ds(column, 128)], ref[a].at[:, k, y], which, 2)
    for a in range(3):
        load(master[a], held_master[a], 3, 4)
        load(moment[a], held_moment[a], 3, 4)

    pl.semaphore_wait(barrier, 4)

    mate = ys[1]
    place = {"both": both, "mate": mate, "mine": yh}
    loaded = set()
    for step, (chunk, ks, y) in enumerate(ORDER):
        for k in ks:
            which = (2, 1, 0, 1)[k] if step else 4
            if which not in loaded:
                loaded.add(which)
                wait_bytes(load_sem.at[which], load_bytes[which])
        for p in chunk:
            for k in ks:
                send(
                    at(give, p, both, k, place[y]),
                    at(peer, p, both, k, place[y]),
                    core_to,
                    ("core", min(step, LAST)),
                    0,
                )

    paired = set()

    def pair(step):
        chunk, ks, y = ORDER[step]
        if min(step, LAST) not in paired:
            paired.add(min(step, LAST))
            arrive("core", min(step, LAST))
        for p in chunk:
            for k in ks:
                total = at(own, p, both, k, place[y])
                total[...] = total[...] + at(peer, p, both, k, place[y])[...]

    def total_of(*pieces):
        return sum(piece.astype(f32) for piece in pieces)

    layers = range(LAYERS)

    def zy_far(chunk):
        for l in layers:
            for p in chunk:
                send(at(own, p, l, 2, both), far[p].at[l], z_to[up[l]], ("far", chunk), 1)

    def zy_direct(chunk):
        for l in layers:
            for p in chunk:
                k = down[l]
                send(at(own, p, l, k, both), direct[p].at[l], z_to[k], ("final", chunk), 1)

    def zy_pass_on(chunk):
        arrive("far", chunk)
        for l in layers:
            for p in chunk:
                k = up[l]
                total = at(own, p, l, k, both)
                total[...] = total_of(total[...], far[p][l]).astype(bf16)
                send(total, summed[p].at[l], z_to[k], ("final", chunk), 1)

    def zy_across(chunk):
        arrive("final", chunk)
        for p in chunk:
            for l in layers:
                total = at(own, p, l, 0, mate)
                total[...] = total_of(total[...], direct[p][l, mate], summed[p][l, mate]).astype(
                    bf16
                )
            send(at(own, p, both, 0, mate), across[p].at[:, 0], y_to, ("y", chunk), 1)

    def yz_across(chunk, k):
        group = {0: ("final", chunk), 2: ("far y", chunk)}.get(k, ("side y", chunk))
        for p in chunk:
            send(at(own, p, both, k, mate), across[p].at[:, k], y_to, group, 1)

    def yz_far(chunk):
        arrive("far y", chunk)
        for l in layers:
            for p in chunk:
                total = at(own, p, l, 2, yh)
                total[...] = total[...] + across[p][l, 2]
                send(total, far[p].at[l, 0], z_to[up[l]], ("far", chunk), 1)

    def yz_direct(chunk):
        arrive("side y", chunk)
        for l in layers:
            for p in chunk:
                k = down[l]
                total = at(own, p, l, k, yh)
                total[...] = total[...] + across[p][l, k]
                send(total, direct[p].at[l, 0], z_to[k], ("final", chunk), 1)

    def yz_pass_on(chunk):
        arrive("far", chunk)
        for l in layers:
            for p in chunk:
                k = up[l]
                total = at(own, p, l, k, yh)
                total[...] = total_of(total[...], across[p][l, k], far[p][l, 0]).astype(bf16)
                send(total, summed[p].at[l, 0], z_to[k], ("final", chunk), 1)

    state_here = []

    def update(chunk):
        if not state_here:
            wait_bytes(load_sem.at[3], load_bytes[3])
            state_here.append(True)
        if chunk in Z_FIRST:
            arrive("y", chunk)
        else:
            arrive("final", chunk)
        for p in chunk:
            a, first, rows = PARTS[p]
            for l in layers:
                here = (l, pl.ds(first, rows))
                j = yh if chunk in Z_FIRST else 0
                total = total_of(
                    at(own, p, l, 0, yh)[...], direct[p][l, j], summed[p][l, j], across[p][l, 0]
                )
                average = total * (1.0 / REPLICAS)
                momentum = OUTER_MOMENTUM * held_moment[a][here] + average
                updated = held_master[a][here] - OUTER_RATE * (
                    average + OUTER_MOMENTUM * momentum
                )
                new_moment[a][here] = momentum
                new_master[a][here] = updated
                block(params, p, l, yh, z, c)[...] = updated.astype(bf16)

    def share(p, l, y, zz, to, group, which=2):
        piece = block(params, p, l, y, zz, c)
        send(piece, piece, to, group, which)

    def core_share(p, l, j, k):
        share(p, l, ys[j], zs[k], core_to, ("core",), 3)

    def gather_z(chunk, j):
        for name, way in (("up", up), ("down", down)):
            for l in layers:
                for p in chunk:
                    share(p, l, ys[j], z, z_to[way[l]], (name, chunk, j))

    def gather_own(chunk, j):
        for p in chunk:
            core_share(p, both, j, 0)

    def gather_y(chunk):
        for p in chunk:
            share(p, both, yh, z, y_to, ("across", chunk, "own"))

    def came(chunk, j, name):
        arrive(name, chunk, j)
        for l in layers:
            k = {"up": down[l], "down": up[l], "on": 2}[name]
            for p in chunk:
                if name == "up":
                    share(p, l, ys[j], zs[k], z_to[up[l]], ("on", chunk, j))
        for l in layers:
            k = {"up": down[l], "down": up[l], "on": 2}[name]
            for p in chunk:
                if chunk in Y_FIRST:
                    share(p, l, yh, zs[k], y_to, ("across", chunk, name))
                core_share(p, l, j, k)

    def came_across(chunk, name):
        arrive("across", chunk, name)
        for l in layers:
            k = {"own": 0, "up": down[l], "down": up[l], "on": 2}[name]
            for p in chunk:
                core_share(p, l, 1, k)

    stages = dict(
        pair=pair,
        zy_far=zy_far,
        zy_direct=zy_direct,
        zy_pass_on=zy_pass_on,
        zy_across=zy_across,
        yz_across=yz_across,
        yz_far=yz_far,
        yz_direct=yz_direct,
        yz_pass_on=yz_pass_on,
        update=update,
        gather_y=gather_y,
        gather_z=gather_z,
        gather_own=gather_own,
        came=came,
        came_across=came_across,
    )
    for name, *rest in SCHEDULE:
        stages[name](*rest)
    arrive("core")
    for which in range(SENDS):
        wait_bytes(send_sem.at[which], sent[which])


def write_kernel(*refs):
    sources, results, sem = refs[:9], refs[9:18], refs[18]
    copies = []
    for source, result in zip(sources, results):
        for layer in range(LAYERS):
            copies.append(
                pltpu.make_async_copy(source.at[layer], result.at[layer], sem.at[len(copies)])
            )
    for i, copy in enumerate(copies):
        copy.start(priority=i % 2)
    for copy in copies:
        copy.wait()


def outer_step(
    delta_query,
    master_query,
    moment_query,
    delta_latent,
    master_latent,
    moment_latent,
    delta_output,
    master_output,
    moment_output,
):
    f32, bf16 = jnp.float32, jnp.bfloat16
    shapes = []
    for a, block in enumerate(BLOCKS):
        whole = (LAYERS, 2, 4, 2, *block) if a < 2 else (LAYERS, block[0], 16 * block[1])
        shapes += [(whole, bf16), ((LAYERS, *block), f32), ((LAYERS, *block), f32)]
    z_first = {p for chunk in Z_FIRST for p in chunk}
    scratch = []
    scratch += [pltpu.VMEM((LAYERS, 4, 2, *block), bf16) for _ in range(3) for block in BLOCKS]
    for kind in range(4):
        for p in range(len(PARTS)):
            if kind < 3:
                lead = (LAYERS, 2 if p in z_first else 1)
            else:
                lead = (LAYERS, 1 if p in z_first else 4)
            scratch.append(pltpu.VMEM((*lead, *part_shape(p)), bf16))
    scratch += [pltpu.VMEM((LAYERS, *block), f32) for _ in range(2) for block in BLOCKS]
    operands = (
        delta_query.reshape(shapes[0][0]),
        master_query,
        moment_query,
        delta_latent.reshape(shapes[3][0]),
        master_latent,
        moment_latent,
        delta_output.reshape(shapes[6][0]),
        master_output,
        moment_output,
    )
    operands = [pltpu.with_memory_space_constraint(x, pltpu.HBM) for x in operands]
    results = pl.pallas_call(
        outer_kernel,
        out_shape=tuple(pltpu.VMEM(*shape) for shape in shapes),
        in_specs=[pl.BlockSpec(memory_space=pltpu.HBM)] * 9,
        out_specs=tuple(pl.BlockSpec(memory_space=pltpu.VMEM) for _ in range(9)),
        scratch_shapes=scratch
        + [
            pltpu.VMEM((SIZE_ROWS, 128), bf16),
            pltpu.SemaphoreType.DMA((LOADS,)),
            pltpu.SemaphoreType.DMA((SENDS,)),
            pltpu.SemaphoreType.DMA((GROUPS,)),
        ],
        compiler_params=pltpu.CompilerParams(
            collective_id=0, has_side_effects=True, vmem_limit_bytes=40 * 1024 * 1024
        ),
    )(*operands)
    results = [pltpu.with_memory_space_constraint(x, pltpu.VMEM) for x in results]
    results = pl.pallas_call(
        write_kernel,
        out_shape=tuple(pltpu.HBM(*shape) for shape in shapes),
        in_specs=[pl.BlockSpec(memory_space=pltpu.VMEM)] * 9,
        out_specs=tuple(pl.BlockSpec(memory_space=pltpu.HBM) for _ in range(9)),
        scratch_shapes=[pltpu.SemaphoreType.DMA((9 * LAYERS,))],
        compiler_params=pltpu.CompilerParams(vmem_limit_bytes=4 * 1024 * 1024),
    )(*results)
    query, latent = results[0], results[3]
    return (
        query.reshape(LAYERS, 2048, 384),
        *results[1:3],
        latent.reshape(LAYERS, 512, 512),
        *results[4:],
    )


def solution(mesh):
    torus = Mesh(mesh.devices.reshape(2, 4, 2, 2, 4), (*REP, *TP))
    return jax.shard_map(
        outer_step,
        mesh=torus,
        in_specs=(
            P(REP, None, None, TP),
            P(None, REP, TP),
            P(None, REP, TP),
            P(REP, None, None, TP),
            P(None, REP, TP),
            P(None, REP, TP),
            P(REP, None, TP, None),
            P(None, TP, REP),
            P(None, TP, REP),
        ),
        out_specs=(
            P(None, None, TP),
            P(None, REP, TP),
            P(None, REP, TP),
            P(None, None, TP),
            P(None, REP, TP),
            P(None, REP, TP),
            P(None, TP, None),
            P(None, TP, REP),
            P(None, TP, REP),
        ),
        check_vma=False,
    )
```
